256 devices in a mesh: dop: 32 (over z, y), slow: 8 (over x, core).
Axes of the slice: x: 4, y: 4, z: 8, core: 2. Of those that a mesh axis runs over, the one named last changes fastest.
Arguments:
- profiles: bfloat16 [64, 2, 1024, 2048], P('slow', None, 'dop'), may hold values from -6 to 6
- range_walk: int32 [2048], replicated, may hold values from -32 to 32
- band_order: int32 [256], replicated, may hold values from 0 to 255, each once
Outputs:
- ambiguity: float32 [2048, 1024], P(('dop', 'slow'))
The draws below stay inside these ranges and needn't reach their ends.
Inputs may be any that keep to these rules, and one draw needn't show every extreme that they name: `band_order`: each band number appears exactly once.
All inputs are finite; a program needn't handle non-finite values.
Results may differ from the reference program's by a relative error of at most 0.00067.
Values sent between devices are 32-bit elements; how exact they have to be, the bound alone decides.
No kernel may reach another device: no remote copies, remote signals or barrier semaphores. Data moves between devices by JAX's collectives and lax.ppermute only.
A program may use at most 64 MiB of HBM per device.

```python
import math
import jax
import jax.numpy as jnp
from jax import lax

F = 2048
R = 1024
WALK = 32
BATCHES = 64
BANDS = 256
BAND_ROWS = 8


def plant(result, own_key, smallest, top_value):
    dims = result.shape
    index_at = [jax.random.randint(jax.random.fold_in(own_key, axis), (), 0, dims[axis]) for axis in range(len(dims))]
    result = result.at[tuple(index_at)].set(smallest)
    longest = dims.index(max(dims))
    index_at[longest] = (index_at[longest] + 1) % dims[longest]
    return result.at[tuple(index_at)].set(top_value)


def steps_of(own_key, shape, cuts, least, top_value):
    factor_of = 1.0
    for axis_at, blocks in cuts:
        heights = jax.random.uniform(jax.random.fold_in(jax.random.fold_in(own_key, 6), axis_at), (blocks,), jnp.float32, least / len(cuts), top_value / len(cuts))
        factor_of = factor_of * jnp.repeat(jnp.exp(heights), shape[axis_at] // blocks).reshape((-1,) + (1,) * (len(shape) - 1 - axis_at))
    return factor_of


def bell_draw(key, extent, deviation, bound, split=(), held_as=jnp.bfloat16):
    drawn = deviation * jax.random.normal(key, extent, jnp.float32)
    if split:
        drawn = drawn * steps_of(key, extent, split, -0.22, 0.18)
    return jnp.clip(drawn, -bound, bound).astype(held_as)


def setup_inputs(seed: int = 0) -> dict:
    streams_of = jax.random.split(jax.random.key(seed), 4)
    profiles = bell_draw(streams_of[0], (BATCHES, 2, R, F), 1.0, 6.0, ((0, 8), (2, 32)))
    range_walk = plant(jax.random.randint(streams_of[1], (F,), -WALK, WALK + 1), jax.random.fold_in(streams_of[1], 1), -WALK, WALK).astype(jnp.int32)
    band_order = jax.random.permutation(streams_of[2], BANDS).astype(jnp.int32)
    return dict(profiles=profiles, range_walk=range_walk, band_order=band_order)


def fourier_tables(length):
    counter = jnp.arange(length, dtype=jnp.int32)
    phases = (counter[:, None] * counter[None, :]) % length
    angles = phases.astype(jnp.float32) * (2.0 * math.pi / length)
    return jnp.cos(angles).astype(jnp.bfloat16), jnp.sin(angles).astype(jnp.bfloat16)


def batch_powers(block, cosine, sine_table):
    count = block.shape[0]
    delays = block.shape[2]
    bins = block.shape[3]
    stacked = block.reshape(count * 2 * delays, bins)
    first = jnp.dot(stacked, cosine, preferred_element_type=jnp.float32).reshape(count, 2, delays, bins)
    second = jnp.dot(stacked, sine_table, preferred_element_type=jnp.float32).reshape(count, 2, delays, bins)
    real_part = first[:, 0] + second[:, 1]
    imag_part = first[:, 1] - second[:, 0]
    return real_part * real_part + imag_part * imag_part


def reference(profiles, range_walk, band_order):
    cosine, sine_table = fourier_tables(F)

    def accumulate(running, inputs):
        block, batch = inputs
        powers = batch_powers(block[None], cosine, sine_table)[0]
        offsets = (range_walk * batch) // BATCHES
        padded = jnp.pad(powers, ((WALK, WALK), (0, 0)))
        lookup = jnp.arange(R, dtype=jnp.int32)[:, None] + offsets[None, :] + WALK
        aligned = jnp.take_along_axis(padded, lookup.astype(jnp.int32), axis=0)
        return running + aligned, jnp.zeros((), jnp.float32)

    start = jnp.zeros((R, F), jnp.float32)
    scanned = lax.scan(accumulate, start, (profiles, jnp.arange(BATCHES, dtype=jnp.int32)))
    power_map = (scanned[0] * (1.0 / (BATCHES * F))).T
    ordered = jnp.take(power_map.reshape(BANDS, BAND_ROWS, R), band_order, axis=0)
    return ordered.reshape(F, R)
```

```python
import functools
import math

import jax
import jax.numpy as jnp
from jax import lax
from jax.experimental import pallas as pl
from jax.experimental.pallas import tpu as pltpu
from jax.sharding import PartitionSpec as P

WALK = 32
F = 2048
BANDS = 256
ROWS = 32
PER = 8
WIN = 40
SCALE = 1.0 / (64 * F)


def shifted(value, rows):
    if rows == 0:
        return value
    return pltpu.roll(value, rows, 0)


def spectra_kernel(slow_ref, x_ref, order_ref, walk_ref, out_ref, hi_ref, lo_ref, w_ref, kept_ref):
    slow = slow_ref[0]
    pulse = lax.broadcasted_iota(jnp.int32, (BANDS, BANDS), 0)
    turns = (pulse * order_ref[...]) & (BANDS - 1)
    angle = turns.astype(jnp.float32) * (2.0 * math.pi / BANDS)
    band_cos = jnp.cos(angle)
    band_sin = jnp.sin(angle)
    rows512 = lax.broadcasted_iota(jnp.int32, (512, 1), 0)
    walks = walk_ref[...]
    first = (walks * (8 * slow)) >> 6
    lead = jnp.where(walks >= 0, 4, 0)
    moves = [lead - (((walks * (8 * slow + g)) >> 6) - first) for g in range(PER)]
    for q in range(4):
        for g in range(PER):
            part = [
                [x_ref[g, c, :, k * 512 : (k + 1) * 512].astype(jnp.float32) for k in range(4)]
                for c in range(2)
            ]
            re, im = part
            if q % 2 == 0:
                zr = (re[0] + re[2]) + (re[1] + re[3]) * (1.0 if q == 0 else -1.0)
                zi = (im[0] + im[2]) + (im[1] + im[3]) * (1.0 if q == 0 else -1.0)
            else:
                sign = 1.0 if q == 1 else -1.0
                zr = (re[0] - re[2]) + (im[1] - im[3]) * sign
                zi = (im[0] - im[2]) - (re[1] - re[3]) * sign
            rh = zr.astype(jnp.bfloat16)
            ih = zi.astype(jnp.bfloat16)
            rl = (zr - rh.astype(jnp.float32)).astype(jnp.bfloat16)
            il = (zi - ih.astype(jnp.float32)).astype(jnp.bfloat16)
            up = slice(g * ROWS, (g + 1) * ROWS)
            down = slice(256 + g * ROWS, 256 + (g + 1) * ROWS)
            hi_ref[q, up, 0:512] = rh
            hi_ref[q, up, 512:1024] = ih
            hi_ref[q, down, 0:512] = ih
            hi_ref[q, down, 512:1024] = -rh
            lo_ref[q, up, 0:512] = rl
            lo_ref[q, up, 512:1024] = il
            lo_ref[q, down, 0:512] = il
            lo_ref[q, down, 512:1024] = -rl
        for jj in range(2):
            j = q + 4 * jj
            fine = ((rows512 * j) & (F - 1)).astype(jnp.float32) * (2.0 * math.pi / F)
            fine_cos = jnp.cos(fine)
            fine_sin = jnp.sin(fine)
            for half in range(2):
                fc = fine_cos[half * 256 : (half + 1) * 256]
                fs = fine_sin[half * 256 : (half + 1) * 256]
                at = half * 256
                w_ref[j, at : at + 256, :] = (band_cos * fc - band_sin * fs).astype(jnp.bfloat16)
                w_ref[j, 512 + at : 512 + at + 256, :] = (band_sin * fc + band_cos * fs).astype(
                    jnp.bfloat16
                )
            w = w_ref[j]
            spec = jnp.dot(hi_ref[q], w, preferred_element_type=jnp.float32)
            spec = spec + jnp.dot(lo_ref[q], w, preferred_element_type=jnp.float32)
            powers = spec[:256] * spec[:256] + spec[256:] * spec[256:]
            classes = [jnp.zeros((ROWS, BANDS), jnp.float32) for _ in range(5)]
            for g in range(PER):
                own = powers[g * ROWS : (g + 1) * ROWS]
                move = moves[g][j : j + 1, :]
                for k in range(5):
                    classes[k] = classes[k] + jnp.where(move == k, own, 0.0)
            rim = jnp.zeros((WIN - ROWS, BANDS), jnp.float32)
            total = None
            for k in range(5):
                piece = shifted(jnp.concatenate([classes[k], rim], axis=0), k)
                total = piece if total is None else total + piece
            kept_ref[j] = total
    lane = lax.broadcasted_iota(jnp.int32, (WIN, 128), 1) // 32
    for quad in range(2):
        for tile in range(2):
            held = [kept_ref[4 * tile + c, :, quad * 128 : (quad + 1) * 128] for c in range(4)]
            for s in range(4):
                result = None
                for c in range(4):
                    turned = held[c]
                    if c != s:
                        turned = pltpu.roll(turned, ((c - s) % 4) * 32, 1)
                    result = turned if result is None else jnp.where(lane == c, turned, result)
                out_ref[4 * quad + s, :, tile * 128 : (tile + 1) * 128] = result


def slow_kernel(x_ref, walk_ref, out_ref, turned_ref):
    walks = walk_ref[...]
    base = jnp.where(walks >= 0, 28, 32)
    for tile in range(2):
        lanes = slice(tile * 128, (tile + 1) * 128)
        total = jnp.zeros((96, 128), jnp.float32)
        for source in range(8):
            move = base - ((walks * source) >> 3)
            current = x_ref[source, :, lanes]
            rows = 48
            current = jnp.concatenate([current, jnp.zeros((rows - WIN, 128), jnp.float32)], axis=0)
            for bit in range(6):
                taken = ((move >> bit) & 1)[:, lanes] == 1
                if bit >= 3:
                    pad = jnp.zeros((1 << bit, 128), jnp.float32)
                    low = jnp.concatenate([current, pad], axis=0)
                    high = jnp.concatenate([pad, current], axis=0)
                    if low.shape[0] > 96:
                        low, high = low[:96], high[:96]
                    current = jnp.where(taken, high, low)
                else:
                    current = jnp.where(taken, pltpu.roll(current, 1 << bit, 0), current)
            total = total + current[:96]
        total = jnp.concatenate([total, jnp.zeros((32, 128), jnp.float32)], axis=0) * SCALE
        turned_ref[lanes, :] = total.T
    for block in range(32):
        out_ref[block] = turned_ref[pl.ds(block, 8, stride=32), :]


def join_kernel(x_ref, out_ref):
    lane = lax.broadcasted_iota(jnp.int32, (8, 128), 1)
    for v in range(8):
        total = None
        for step in range(-1, 5):
            block = 4 * v + step
            if block < 0 or block >= 32:
                continue
            offset = 32 * (step - 1)
            piece = x_ref[block]
            if offset != 0:
                piece = pltpu.roll(piece, offset % 128, 1)
            if offset < 0:
                piece = jnp.where(lane < 96 + offset, piece, 0.0)
            elif offset > 0:
                piece = jnp.where(lane >= offset, piece, 0.0)
            total = piece if total is None else total + piece
        out_ref[:, v * 128 : (v + 1) * 128] = total


VM = pl.BlockSpec(memory_space=pltpu.VMEM)
SM = pl.BlockSpec(memory_space=pltpu.SMEM)


def on_device(profiles, range_walk, band_order):
    slow = lax.axis_index("slow")
    order = band_order.reshape(32, 8).T.reshape(1, BANDS)
    walks = jnp.take(range_walk.reshape(BANDS, 8), order[0], axis=0).T
    sums = pl.pallas_call(
        spectra_kernel,
        out_shape=jax.ShapeDtypeStruct((8, WIN, BANDS), jnp.float32),
        in_specs=[SM, VM, VM, VM],
        out_specs=VM,
        scratch_shapes=[
            pltpu.VMEM((4, 512, 1024), jnp.bfloat16),
            pltpu.VMEM((4, 512, 1024), jnp.bfloat16),
            pltpu.VMEM((8, 1024, 256), jnp.bfloat16),
            pltpu.VMEM((8, WIN, BANDS), jnp.float32),
        ],
    )(slow.reshape(1), profiles, order, walks)
    gathered = lax.all_to_all(sums, "slow", split_axis=0, concat_axis=0, tiled=True)
    own = lax.dynamic_slice(walks, (0, slow * 32), (8, 32)).reshape(1, BANDS)
    blocks = pl.pallas_call(
        slow_kernel,
        out_shape=jax.ShapeDtypeStruct((32, 8, 128), jnp.float32),
        in_specs=[VM, VM],
        out_specs=VM,
        scratch_shapes=[pltpu.VMEM((BANDS, 128), jnp.float32)],
    )(gathered, own)
    arrived = lax.all_to_all(blocks, "dop", split_axis=0, concat_axis=0, tiled=True)
    return pl.pallas_call(
        join_kernel,
        out_shape=jax.ShapeDtypeStruct((8, 1024), jnp.float32),
        in_specs=[VM],
        out_specs=VM,
    )(arrived)


def solution(mesh):
    placed = (P("slow", None, "dop", None), P(), P())
    return jax.shard_map(
        on_device, mesh=mesh, in_specs=placed, out_specs=P(("dop", "slow"), None), check_vma=False
    )
```

```python
import math

import jax
import jax.numpy as jnp
from jax import lax
from jax.experimental import pallas as pl
from jax.experimental.pallas import tpu as pltpu
from jax.sharding import Mesh, PartitionSpec as P

F = 2048
BANDS = 256
ROWS = 32
PER = 8
WIN = 40
SCALE = 1.0 / (64 * F)
f32 = jnp.float32
bf16 = jnp.bfloat16


def cos_sin(turns, period):
    quarter = period // 4
    shift = quarter.bit_length() - 1
    quad = (turns + quarter // 2) >> shift
    r = (turns - (quad << shift)).astype(f32) * (2.0 * math.pi / period)
    r2 = r * r
    c = 1.0 + r2 * (-1 / 2 + r2 * (1 / 24 + r2 * (-1 / 720 + r2 * (1 / 40320))))
    s = r * (1.0 + r2 * (-1 / 6 + r2 * (1 / 120 + r2 * (-1 / 5040 + r2 * (1 / 362880)))))
    odd = (quad & 1) == 1
    cosine = jnp.where(odd, s, c)
    sine = jnp.where(odd, c, s)
    cosine = jnp.where(((quad + 1) & 2) == 2, -cosine, cosine)
    sine = jnp.where((quad & 2) == 2, -sine, sine)
    return cosine, sine


def iota(shape, dim):
    return lax.broadcasted_iota(jnp.int32, shape, dim)


def spectra_kernel(
    place_ref, x_hbm, order_ref, walk_ref, send_ref, keep_ref, meet_ref,
    x_ref, odd_ref, even_ref, wodd_ref, weven_ref, sems,
):
    slow = place_ref[0]
    core = place_ref[1]
    copies = [pltpu.make_async_copy(x_hbm.at[g], x_ref.at[g], sems.at[g]) for g in range(PER)]
    for copy in copies:
        copy.start()

    order = order_ref[...].astype(f32).astype(bf16)
    halves = []
    for c in range(2):
        owner = ((iota((128, 128), 1) & 31) << 3) + ((iota((128, 128), 1) >> 5) << 1) + c
        pick = iota((128, 128), 0) == (owner & 127)
        got = jnp.dot(order, pick.astype(f32).astype(bf16), preferred_element_type=f32)
        halves.append(jnp.where((iota((1, 128), 1) & 31) < 16, got[0:1], got[1:2]))
    flip = core == 0
    bands = jnp.concatenate(
        [jnp.where(flip, halves[1], halves[0]), jnp.where(flip, halves[0], halves[1])], axis=1
    ).astype(jnp.int32)

    band_cos, band_sin = cos_sin((iota((BANDS, BANDS), 0) * bands) & (BANDS - 1), BANDS)
    fine_cos, fine_sin = cos_sin((iota((512, 128), 0) * (iota((512, 128), 1) & 7)) & (F - 1), F)

    def table(j):
        for half in range(2 if j % 2 else 1):
            at = half * 256
            fc = fine_cos[at : at + 256, j : j + 1]
            fs = fine_sin[at : at + 256, j : j + 1]
            c = (band_cos * fc - band_sin * fs).astype(bf16)
            s = (band_sin * fc + band_cos * fs).astype(bf16)
            if j % 2:
                wodd_ref[j // 2, at : at + 256, :] = c
                wodd_ref[j // 2, 512 + at : 512 + at + 256, :] = s
            else:
                weven_ref[j // 2, 0:256, :] = c
                weven_ref[j // 2, 256:512, :] = s

    def put(ref, index, row, col, depth, zr, zi):
        rh = zr.astype(bf16)
        ih = zi.astype(bf16)
        rl = (zr - rh.astype(f32)).astype(bf16)
        il = (zi - ih.astype(f32)).astype(bf16)
        for level, (re, im) in enumerate(((rh, ih), (rl, il))):
            ref[index, level, row : row + 16, col : col + 128] = re
            ref[index, level, row : row + 16, depth + col : depth + col + 128] = im
            ref[index, level, 256 + row : 256 + row + 16, col : col + 128] = im
            ref[index, level, 256 + row : 256 + row + 16, depth + col : depth + col + 128] = -re

    def fold(g, part, pair):
        zs = []
        for cb in (pair, pair + 2):
            re, im = [
                [
                    x_ref[
                        g, c, part * 16 : part * 16 + 16, k * 512 + cb * 128 : k * 512 + cb * 128 + 128
                    ].astype(f32)
                    for k in range(4)
                ]
                for c in range(2)
            ]
            s02r, s02i = re[0] + re[2], im[0] + im[2]
            d02r, d02i = re[0] - re[2], im[0] - im[2]
            s13r, s13i = re[1] + re[3], im[1] + im[3]
            d13r, d13i = re[1] - re[3], im[1] - im[3]
            row = g * ROWS + part * 16
            put(odd_ref, 0, row, cb * 128, 512, d02r + d13i, d02i - d13r)
            put(odd_ref, 1, row, cb * 128, 512, d02r - d13i, d02i + d13r)
            zs.append((s02r + s13r, s02i + s13i, s02r - s13r, s02i - s13i))
        (ar, ai, cr, ci), (br, bi, dr, di) = zs
        put(even_ref, 0, row, pair * 128, 256, ar + br, ai + bi)
        put(even_ref, 2, row, pair * 128, 256, ar - br, ai - bi)
        put(even_ref, 1, row, pair * 128, 256, cr + di, ci - dr)
        put(even_ref, 3, row, pair * 128, 256, cr - di, ci + dr)

    rows16 = iota((16, BANDS), 0) == (bands >> 4)
    walks = []
    for j in range(8):
        pick = iota((128, BANDS), 0) == (((bands & 15) << 3) + j)
        got = jnp.dot(
            walk_ref[...].astype(f32).astype(bf16),
            pick.astype(f32).astype(bf16),
            preferred_element_type=f32,
        )
        walks.append(jnp.sum(jnp.where(rows16, got, 0.0), axis=0, keepdims=True).astype(jnp.int32))

    def align(j, spec):
        powers = spec[:256] * spec[:256] + spec[256:] * spec[256:]
        walk = walks[j]
        ahead = walk >= 0
        at = [(walk * (8 * slow + g)) >> 6 for g in range(PER)]
        rim = jnp.zeros((WIN - ROWS, BANDS), f32)
        total = None
        for i in range(PER):
            own = jnp.where(
                ahead, powers[i * ROWS : (i + 1) * ROWS], powers[(7 - i) * ROWS : (8 - i) * ROWS]
            )
            own = jnp.concatenate([own, rim], axis=0)
            if i == 0:
                total = own
            else:
                step = jnp.where(ahead, at[i] - at[i - 1], at[7 - i] - at[8 - i]) == 1
                total = jnp.where(step, pltpu.roll(total, 1, 0), total) + own
        send_ref[j] = total[:, :128]
        keep_ref[j] = total[:, 128:]
        meet = walk[:, 128:]
        lower = slow & ~1
        apart = jnp.where(
            meet >= 0,
            ((meet * (8 * lower + 15)) >> 6) - ((meet * (8 * lower + 7)) >> 6),
            ((meet * (8 * lower)) >> 6) - ((meet * (8 * lower + 8)) >> 6),
        )
        meet_ref[j : j + 1, :] = jnp.where(meet >= 0, apart, -apart - 1)

    for j in range(8):
        table(j)
    for g in range(PER):
        copies[g].wait()
        for part in range(2):
            for pair in range(2):
                fold(g, part, pair)

    def product(j):
        if j % 2:
            left, index, w = odd_ref, (j // 2) % 2, wodd_ref[j // 2]
        else:
            left, index, w = even_ref, j // 2, weven_ref[j // 2]
        return jnp.dot(left[index, 0], w, preferred_element_type=f32) + jnp.dot(
            left[index, 1], w, preferred_element_type=f32
        )

    for j in (1, 5, 3, 7, 0, 2, 4, 6):
        align(j, product(j))


def pair_kernel(place_ref, mine_ref, theirs_ref, meet_ref, out_ref, flat_ref):
    first = place_ref[1] == 0
    for j in range(8):
        mine = mine_ref[j]
        theirs = theirs_ref[j]
        lower = jnp.where(first, mine, theirs)
        upper = jnp.where(first, theirs, mine)
        meet = meet_ref[j : j + 1, :]
        ahead = meet >= 0
        apart = jnp.where(ahead, meet, -meet - 1)
        moved = jnp.where(ahead, lower, upper)
        still = jnp.where(ahead, upper, lower)
        for bit in range(3):
            moved = jnp.where(((apart >> bit) & 1) == 1, pltpu.roll(moved, 1 << bit, 0), moved)
        flat_ref[j * WIN : (j + 1) * WIN, :] = moved + still
    flat_ref[8 * WIN :, :] = jnp.zeros((64, 128), f32)
    for piece in range(3):
        part = slice(piece * 128, (piece + 1) * 128)
        out_ref[:, part] = flat_ref[part, :].T


def join_kernel(place_ref, order_ref, walk_ref, x_ref, out_ref, turned_ref):
    owner = place_ref[2]
    band = order_ref[owner]
    lane = iota((1, 128), 1)
    group = lane // 32
    block = lane & 31
    flat = jnp.concatenate(
        [x_ref[:, piece * 128 : (piece + 1) * 128].T for piece in range(3)], axis=0
    )
    for quad in range(2):
        packed = None
        for jq in range(4):
            j = quad * 4 + jq
            walk = walk_ref[band * 8 + j]
            last = jnp.where(walk >= 0, 15, 0)
            move = jnp.zeros((1, 128), jnp.int32)
            for x in range(4):
                move = jnp.where(group == x, 32 - ((walk * (16 * x + last)) >> 6), move)
            current = jnp.concatenate(
                [flat[j * WIN : (j + 1) * WIN], jnp.zeros((8, 128), f32)], axis=0
            )
            for bit in range(6):
                taken = ((move >> bit) & 1) == 1
                if bit < 3:
                    current = jnp.where(taken, pltpu.roll(current, 1 << bit, 0), current)
                else:
                    pad = jnp.zeros((1 << bit, 128), f32)
                    low = jnp.concatenate([current, pad], axis=0)
                    high = jnp.concatenate([pad, current], axis=0)
                    current = jnp.where(taken, high[:96], low[:96])
            current = current + pltpu.roll(current, 64, 1)
            current = current + pltpu.roll(current, 32, 1)
            before = jnp.where(block == 31, 0.0, pltpu.roll(current[0:32], 127, 1))
            after = jnp.where(block == 0, 0.0, pltpu.roll(current[64:96], 1, 1))
            summed = before + current[32:64] + after
            packed = summed if packed is None else jnp.where(group == jq, summed, packed)
        packed = packed * SCALE
        turned_ref[quad * 128 : (quad + 1) * 128, :] = jnp.concatenate([packed] * 4, axis=0).T
    for v in range(8):
        result = None
        for c in range(4):
            piece = turned_ref[pl.ds(4 * v + c, 8, stride=32), :]
            result = piece if result is None else jnp.where(group == c, piece, result)
        out_ref[:, v * 128 : (v + 1) * 128] = result


VM = pl.BlockSpec(memory_space=pltpu.VMEM)
SM = pl.BlockSpec(memory_space=pltpu.SMEM)


def on_device(profiles, range_walk, band_order):
    x, core = lax.axis_index("x"), lax.axis_index("c")
    slow = 2 * x + core
    owner = (lax.axis_index("z") * 4 + lax.axis_index("y")) * 8 + slow
    place = jnp.stack([slow, core, owner]).astype(jnp.int32)
    block = jax.ShapeDtypeStruct((8, WIN, 128), f32)
    send, keep, meet = pl.pallas_call(
        spectra_kernel,
        out_shape=(block, block, jax.ShapeDtypeStruct((8, 128), jnp.int32)),
        in_specs=[SM, pl.BlockSpec(memory_space=pltpu.HBM), VM, VM],
        out_specs=(VM, VM, VM),
        scratch_shapes=[
            pltpu.VMEM((PER, 2, ROWS, F), bf16),
            pltpu.VMEM((2, 2, 512, 1024), bf16),
            pltpu.VMEM((4, 2, 512, 512), bf16),
            pltpu.VMEM((4, 1024, 256), bf16),
            pltpu.VMEM((4, 512, 256), bf16),
            pltpu.SemaphoreType.DMA((PER,)),
        ],
        compiler_params=pltpu.CompilerParams(vmem_limit_bytes=40 << 20),
    )(place, profiles, band_order.reshape(2, 128), range_walk.reshape(16, 128))
    theirs = lax.ppermute(send, "c", [(0, 1), (1, 0)])
    messages = pl.pallas_call(
        pair_kernel,
        out_shape=jax.ShapeDtypeStruct((128, 384), f32),
        in_specs=[SM, VM, VM, VM],
        out_specs=VM,
        scratch_shapes=[pltpu.VMEM((384, 128), f32)],
        compiler_params=pltpu.CompilerParams(vmem_limit_bytes=4 << 20),
    )(place, keep, theirs, meet)
    arrived = lax.all_to_all(
        messages.reshape(128, 1, 384), ("x", "z", "y"), split_axis=0, concat_axis=0, tiled=True
    )
    return pl.pallas_call(
        join_kernel,
        out_shape=jax.ShapeDtypeStruct((8, 1024), f32),
        in_specs=[SM, SM, SM, VM],
        out_specs=VM,
        scratch_shapes=[pltpu.VMEM((256, 128), f32)],
        compiler_params=pltpu.CompilerParams(vmem_limit_bytes=4 << 20),
    )(place, band_order, range_walk, arrived.reshape(128, 384))


def solution(mesh):
    fine = Mesh(mesh.devices.reshape(8, 4, 4, 2), ("z", "y", "x", "c"))
    placed = (P(("x", "c"), None, ("z", "y"), None), P(), P())
    return jax.shard_map(
        on_device, mesh=fine, in_specs=placed, out_specs=P(("z", "y", "x", "c"), None), check_vma=False
    )
```

```python
import math

import jax
import jax.numpy as jnp
from jax import lax
from jax.experimental import pallas as pl
from jax.experimental.pallas import tpu as pltpu
from jax.sharding import Mesh, PartitionSpec as P

F = 2048
BANDS = 256
ROWS = 32
PER = 8
WIN = 40
GRANT = 40 << 20
SCALE = 1.0 / (64 * F)
f32 = jnp.float32
bf16 = jnp.bfloat16


def cos_sin(turns, period):
    quarter = period // 4
    shift = quarter.bit_length() - 1
    quad = (turns + quarter // 2) >> shift
    r = (turns - (quad << shift)).astype(f32) * (2.0 * math.pi / period)
    r2 = r * r
    c = 1.0 + r2 * (-1 / 2 + r2 * (1 / 24 + r2 * (-1 / 720 + r2 * (1 / 40320))))
    s = r * (1.0 + r2 * (-1 / 6 + r2 * (1 / 120 + r2 * (-1 / 5040 + r2 * (1 / 362880)))))
    odd = (quad & 1) == 1
    cosine = jnp.where(odd, s, c)
    sine = jnp.where(odd, c, s)
    cosine = jnp.where(((quad + 1) & 2) == 2, -cosine, cosine)
    sine = jnp.where((quad & 2) == 2, -sine, sine)
    return cosine, sine


def iota(shape, dim):
    return lax.broadcasted_iota(jnp.int32, shape, dim)


def places():
    core = lax.axis_index("c")
    return 2 * lax.axis_index("x") + core, core


def spectra_kernel(
    x_hbm, order_hbm, walk_hbm, send_ref, keep_ref, meet_ref, own_ref,
    x_ref, order_ref, walk_ref, band_ref, fine_ref, sems,
):
    copies = [
        pltpu.make_async_copy(order_hbm, order_ref, sems.at[0]),
        pltpu.make_async_copy(walk_hbm, walk_ref, sems.at[1]),
    ]
    copies += [
        pltpu.make_async_copy(x_hbm.at[g], x_ref.at[g], sems.at[2 + g]) for g in range(PER)
    ]
    for copy in copies:
        copy.start()
    packed = lambda *shape: pltpu.VMEM(shape, bf16)
    pl.run_scoped(
        lambda *refs: spectra(
            copies, send_ref, keep_ref, meet_ref, own_ref,
            x_ref, order_ref, walk_ref, band_ref, fine_ref, *refs
        ),
        packed(2, 2, 512, 1024),
        packed(4, 2, 512, 512),
        packed(4, 1024, 256),
        packed(4, 512, 256),
    )


def spectra(
    copies, send_ref, keep_ref, meet_ref, own_ref,
    x_ref, order_ref, walk_ref, band_ref, fine_ref,
    odd_ref, even_ref, wodd_ref, weven_ref,
):
    slow, core = places()
    for at in range(0, 512, 32):
        fine = cos_sin(((iota((32, 128), 0) + at) * (iota((32, 128), 1) & 7)) & (F - 1), F)
        fine_ref[0, at : at + 32, :] = fine[0]
        fine_ref[1, at : at + 32, :] = fine[1]

    copies[0].wait()
    order = order_ref[...].astype(f32).astype(bf16)
    halves = []
    for c in range(2):
        owner = ((iota((128, 128), 1) & 31) << 3) + ((iota((128, 128), 1) >> 5) << 1) + c
        pick = iota((128, 128), 0) == (owner & 127)
        got = jnp.dot(order, pick.astype(f32).astype(bf16), preferred_element_type=f32)
        halves.append(jnp.where((iota((1, 128), 1) & 31) < 16, got[0:1], got[1:2]))
    flip = core == 0
    bands = jnp.concatenate(
        [jnp.where(flip, halves[1], halves[0]), jnp.where(flip, halves[0], halves[1])], axis=1
    ).astype(jnp.int32)

    for at in range(0, BANDS, 16):
        turns = ((iota((16, BANDS), 0) + at) * bands) & (BANDS - 1)
        band = cos_sin(turns, BANDS)
        band_ref[0, at : at + 16, :] = band[0]
        band_ref[1, at : at + 16, :] = band[1]

    def table(j):
        for half in range(2 if j % 2 else 1):
            for row in range(0, 256, 16):
                at = half * 256 + row
                fc = fine_ref[0, at : at + 16, j : j + 1]
                fs = fine_ref[1, at : at + 16, j : j + 1]
                bc = band_ref[0, row : row + 16, :]
                bs = band_ref[1, row : row + 16, :]
                c = (bc * fc - bs * fs).astype(bf16)
                s = (bs * fc + bc * fs).astype(bf16)
                if j % 2:
                    wodd_ref[j // 2, at : at + 16, :] = c
                    wodd_ref[j // 2, 512 + at : 512 + at + 16, :] = s
                else:
                    weven_ref[j // 2, at : at + 16, :] = c
                    weven_ref[j // 2, 256 + at : 256 + at + 16, :] = s

    def put(ref, index, row, col, depth, zr, zi):
        rh = zr.astype(bf16)
        ih = zi.astype(bf16)
        rl = (zr - rh.astype(f32)).astype(bf16)
        il = (zi - ih.astype(f32)).astype(bf16)
        for level, (re, im) in enumerate(((rh, ih), (rl, il))):
            ref[index, level, row : row + 16, col : col + 128] = re
            ref[index, level, row : row + 16, depth + col : depth + col + 128] = im
            ref[index, level, 256 + row : 256 + row + 16, col : col + 128] = im
            ref[index, level, 256 + row : 256 + row + 16, depth + col : depth + col + 128] = -re

    def quarters(g, part, cb):
        return [
            [
                x_ref[
                    g, c, part * 16 : part * 16 + 16, k * 512 + cb * 128 : k * 512 + cb * 128 + 128
                ].astype(f32)
                for k in range(4)
            ]
            for c in range(2)
        ]

    def fold_odd(g, part, cb):
        re, im = quarters(g, part, cb)
        dr, di = re[0] - re[2], im[0] - im[2]
        er, ei = re[1] - re[3], im[1] - im[3]
        row = g * ROWS + part * 16
        put(odd_ref, 0, row, cb * 128, 512, dr + ei, di - er)
        put(odd_ref, 1, row, cb * 128, 512, dr - ei, di + er)

    def fold_even(g, part, pair):
        row = g * ROWS + part * 16
        zs = []
        for cb in (pair, pair + 2):
            re, im = quarters(g, part, cb)
            sr, si = re[0] + re[2], im[0] + im[2]
            ur, ui = re[1] + re[3], im[1] + im[3]
            zs.append((sr + ur, si + ui, sr - ur, si - ui))
        (ar, ai, cr, ci), (br, bi, dr, di) = zs
        put(even_ref, 0, row, pair * 128, 256, ar + br, ai + bi)
        put(even_ref, 2, row, pair * 128, 256, ar - br, ai - bi)
        put(even_ref, 1, row, pair * 128, 256, cr + di, ci - dr)
        put(even_ref, 3, row, pair * 128, 256, cr - di, ci + dr)

    def walks_of():
        copies[1].wait()
        rows16 = iota((16, BANDS), 0) == (bands >> 4)
        walks = []
        for j in range(8):
            pick = iota((128, BANDS), 0) == (((bands & 15) << 3) + j)
            got = jnp.dot(
                walk_ref[...].astype(f32).astype(bf16),
                pick.astype(f32).astype(bf16),
                preferred_element_type=f32,
            )
            walk = jnp.sum(jnp.where(rows16, got, 0.0), axis=0, keepdims=True).astype(jnp.int32)
            own_ref[j : j + 1, :] = walk[:, 128:]
            walks.append(walk)
        return walks

    def align(j, walk, spec):
        powers = spec[:256] * spec[:256] + spec[256:] * spec[256:]
        ahead = walk >= 0
        at = [(walk * (8 * slow + g)) >> 6 for g in range(PER)]
        rim = jnp.zeros((WIN - ROWS, BANDS), f32)
        total = None
        for i in range(PER):
            own = jnp.where(
                ahead, powers[i * ROWS : (i + 1) * ROWS], powers[(7 - i) * ROWS : (8 - i) * ROWS]
            )
            own = jnp.concatenate([own, rim], axis=0)
            if i == 0:
                total = own
            else:
                step = jnp.where(ahead, at[i] - at[i - 1], at[7 - i] - at[8 - i]) == 1
                total = jnp.where(step, pltpu.roll(total, 1, 0), total) + own
        send_ref[j] = total[:, :128]
        keep_ref[j] = total[:, 128:]
        meet = walk[:, 128:]
        lower = slow & ~1
        apart = jnp.where(
            meet >= 0,
            ((meet * (8 * lower + 15)) >> 6) - ((meet * (8 * lower + 7)) >> 6),
            ((meet * (8 * lower)) >> 6) - ((meet * (8 * lower + 8)) >> 6),
        )
        meet_ref[j : j + 1, :] = jnp.where(meet >= 0, apart, -apart - 1)

    def product(j):
        if j % 2:
            left, index, w = odd_ref, (j // 2) % 2, wodd_ref[j // 2]
        else:
            left, index, w = even_ref, j // 2, weven_ref[j // 2]
        return jnp.dot(left[index, 0], w, preferred_element_type=f32) + jnp.dot(
            left[index, 1], w, preferred_element_type=f32
        )

    walks = walks_of()
    for j in (1, 5, 3, 7, 0, 2, 4, 6):
        table(j)
    for g in range(PER):
        copies[2 + g].wait()
        for part in range(2):
            for cb in range(4):
                fold_odd(g, part, cb)
    for j in (1, 5):
        align(j, walks[j], product(j))
    for g in range(PER):
        for part in range(2):
            for pair in range(2):
                fold_even(g, part, pair)
    for j in (3, 7, 0, 2, 4, 6):
        align(j, walks[j], product(j))


def pair_kernel(mine_ref, theirs_ref, meet_ref, out_ref, flat_ref):
    first = lax.axis_index("c") == 0
    for j in range(8):
        mine = mine_ref[j]
        theirs = theirs_ref[j]
        lower = jnp.where(first, mine, theirs)
        upper = jnp.where(first, theirs, mine)
        meet = meet_ref[j : j + 1, :]
        ahead = meet >= 0
        apart = jnp.where(ahead, meet, -meet - 1)
        moved = jnp.where(ahead, lower, upper)
        still = jnp.where(ahead, upper, lower)
        for bit in range(3):
            moved = jnp.where(((apart >> bit) & 1) == 1, pltpu.roll(moved, 1 << bit, 0), moved)
        flat_ref[j * WIN : (j + 1) * WIN, :] = moved + still
    flat_ref[8 * WIN :, :] = jnp.zeros((64, 128), f32)
    for piece in range(3):
        part = slice(piece * 128, (piece + 1) * 128)
        out_ref[:, part] = flat_ref[part, :].T


def join_kernel(walk_ref, x_ref, out_ref, turned_ref):
    lane = iota((1, 128), 1)
    group = lane // 32
    block = lane & 31
    here = lax.axis_index("x") * 32 + lax.axis_index("z") * 4 + lax.axis_index("y")
    walk = jnp.sum(jnp.where(lane == here, walk_ref[...], 0), axis=1, keepdims=True)
    batch = 16 * group + jnp.where(walk >= 0, 15, 0)
    moves = 32 - ((walk * batch) >> 6)
    flat = jnp.concatenate(
        [x_ref[:, piece * 128 : (piece + 1) * 128].T for piece in range(3)], axis=0
    )
    for quad in range(2):
        packed = None
        for jq in range(4):
            j = quad * 4 + jq
            move = moves[j : j + 1, :]
            current = jnp.concatenate(
                [flat[j * WIN : (j + 1) * WIN], jnp.zeros((8, 128), f32)], axis=0
            )
            for bit in range(6):
                taken = ((move >> bit) & 1) == 1
                if bit < 3:
                    current = jnp.where(taken, pltpu.roll(current, 1 << bit, 0), current)
                else:
                    pad = jnp.zeros((1 << bit, 128), f32)
                    low = jnp.concatenate([current, pad], axis=0)
                    high = jnp.concatenate([pad, current], axis=0)
                    current = jnp.where(taken, high[:96], low[:96])
            current = current + pltpu.roll(current, 64, 1)
            current = current + pltpu.roll(current, 32, 1)
            before = jnp.where(block == 31, 0.0, pltpu.roll(current[0:32], 127, 1))
            after = jnp.where(block == 0, 0.0, pltpu.roll(current[64:96], 1, 1))
            summed = before + current[32:64] + after
            packed = summed if packed is None else jnp.where(group == jq, summed, packed)
        packed = packed * SCALE
        turned_ref[quad * 128 : (quad + 1) * 128, :] = jnp.concatenate([packed] * 4, axis=0).T
    for v in range(8):
        result = None
        for c in range(4):
            piece = turned_ref[pl.ds(4 * v + c, 8, stride=32), :]
            result = piece if result is None else jnp.where(group == c, piece, result)
        out_ref[:, v * 128 : (v + 1) * 128] = result


VM = pl.BlockSpec(memory_space=pltpu.VMEM)


def on_device(profiles, range_walk, band_order):
    block = jax.ShapeDtypeStruct((8, WIN, 128), f32)
    row = jax.ShapeDtypeStruct((8, 128), jnp.int32)
    ANY = pl.BlockSpec(memory_space=pltpu.HBM)
    send, keep, meet, walks = pl.pallas_call(
        spectra_kernel,
        out_shape=(block, block, row, row),
        in_specs=[ANY, ANY, ANY],
        out_specs=(VM, VM, VM, VM),
        scratch_shapes=[
            pltpu.VMEM((PER, 2, ROWS, F), bf16),
            pltpu.VMEM((2, 128), jnp.int32),
            pltpu.VMEM((16, 128), jnp.int32),
            pltpu.VMEM((2, BANDS, BANDS), f32),
            pltpu.VMEM((2, 512, 128), f32),
            pltpu.SemaphoreType.DMA((2 + PER,)),
        ],
        compiler_params=pltpu.CompilerParams(vmem_limit_bytes=GRANT),
    )(
        *(
            pltpu.with_memory_space_constraint(array, pltpu.HBM)
            for array in (profiles, band_order.reshape(2, 128), range_walk.reshape(16, 128))
        )
    )
    theirs = lax.ppermute(send, "c", [(0, 1), (1, 0)])
    messages = pl.pallas_call(
        pair_kernel,
        out_shape=jax.ShapeDtypeStruct((128, 384), f32),
        in_specs=[VM, VM, VM],
        out_specs=VM,
        scratch_shapes=[pltpu.VMEM((384, 128), f32)],
        compiler_params=pltpu.CompilerParams(vmem_limit_bytes=4 << 20),
    )(keep, theirs, meet)
    arrived = lax.all_to_all(
        messages.reshape(128, 1, 384), ("x", "z", "y"), split_axis=0, concat_axis=0, tiled=True
    )
    return pl.pallas_call(
        join_kernel,
        out_shape=jax.ShapeDtypeStruct((8, 1024), f32),
        in_specs=[VM, VM],
        out_specs=VM,
        scratch_shapes=[pltpu.VMEM((256, 128), f32)],
        compiler_params=pltpu.CompilerParams(vmem_limit_bytes=4 << 20),
    )(walks, arrived.reshape(128, 384))


def solution(mesh):
    fine = Mesh(mesh.devices.reshape(8, 4, 4, 2), ("z", "y", "x", "c"))
    placed = (P(("x", "c"), None, ("z", "y"), None), P(), P())
    return jax.shard_map(
        on_device, mesh=fine, in_specs=placed, out_specs=P(("z", "y", "x", "c"), None), check_vma=False
    )
```

```python
import math

import jax
import jax.numpy as jnp
from jax import lax
from jax.experimental import pallas as pl
from jax.experimental.pallas import tpu as pltpu
from jax.sharding import Mesh, PartitionSpec as P

F = 2048
BANDS = 256
ROWS = 32
PER = 8
WIN = 40
GRANT = 40 << 20
SCALE = 1.0 / (64 * F)
f32 = jnp.float32
bf16 = jnp.bfloat16


def cos_sin(turns, period):
    quarter = period // 4
    shift = quarter.bit_length() - 1
    quad = (turns + quarter // 2) >> shift
    r = (turns - (quad << shift)).astype(f32) * (2.0 * math.pi / period)
    r2 = r * r
    c = 1.0 + r2 * (-1 / 2 + r2 * (1 / 24 + r2 * (-1 / 720 + r2 * (1 / 40320))))
    s = r * (1.0 + r2 * (-1 / 6 + r2 * (1 / 120 + r2 * (-1 / 5040 + r2 * (1 / 362880)))))
    odd = (quad & 1) == 1
    cosine = jnp.where(odd, s, c)
    sine = jnp.where(odd, c, s)
    cosine = jnp.where(((quad + 1) & 2) == 2, -cosine, cosine)
    sine = jnp.where((quad & 2) == 2, -sine, sine)
    return cosine, sine


def iota(shape, dim):
    return lax.broadcasted_iota(jnp.int32, shape, dim)


def places():
    core = lax.axis_index("c")
    return 2 * lax.axis_index("x") + core, core


def spectra_kernel(
    x_hbm, order_hbm, walk_hbm, send_ref, keep_ref, meet_ref, own_ref,
    x_ref, order_ref, walk_ref, band_ref, fine_ref, power_ref, sems,
):
    copies = [
        pltpu.make_async_copy(order_hbm, order_ref, sems.at[0]),
        pltpu.make_async_copy(walk_hbm, walk_ref, sems.at[1]),
    ]
    copies += [
        pltpu.make_async_copy(x_hbm.at[g], x_ref.at[g], sems.at[2 + g]) for g in range(PER)
    ]
    for copy in copies:
        copy.start()
    packed = lambda *shape: pltpu.VMEM(shape, bf16)
    pl.run_scoped(
        lambda *refs: spectra(
            copies, send_ref, keep_ref, meet_ref, own_ref,
            x_ref, order_ref, walk_ref, band_ref, fine_ref, power_ref, *refs
        ),
        packed(2, 2, 512, 1024),
        packed(4, 2, 512, 512),
        packed(4, 1024, 256),
        packed(4, 512, 256),
    )


def spectra(
    copies, send_ref, keep_ref, meet_ref, own_ref,
    x_ref, order_ref, walk_ref, band_ref, fine_ref, power_ref,
    odd_ref, even_ref, wodd_ref, weven_ref,
):
    slow, core = places()
    for at in range(0, 512, 32):
        fine = cos_sin(((iota((32, 128), 0) + at) * (iota((32, 128), 1) & 7)) & (F - 1), F)
        fine_ref[0, at : at + 32, :] = fine[0]
        fine_ref[1, at : at + 32, :] = fine[1]

    copies[0].wait()
    order = order_ref[...].astype(f32).astype(bf16)
    halves = []
    for c in range(2):
        owner = ((iota((128, 128), 1) & 31) << 3) + ((iota((128, 128), 1) >> 5) << 1) + c
        pick = iota((128, 128), 0) == (owner & 127)
        got = jnp.dot(order, pick.astype(f32).astype(bf16), preferred_element_type=f32)
        halves.append(jnp.where((iota((1, 128), 1) & 31) < 16, got[0:1], got[1:2]))
    flip = core == 0
    bands = jnp.concatenate(
        [jnp.where(flip, halves[1], halves[0]), jnp.where(flip, halves[0], halves[1])], axis=1
    ).astype(jnp.int32)

    for at in range(0, BANDS, 16):
        turns = ((iota((16, BANDS), 0) + at) * bands) & (BANDS - 1)
        band = cos_sin(turns, BANDS)
        band_ref[0, at : at + 16, :] = band[0]
        band_ref[1, at : at + 16, :] = band[1]

    def table(j, half, row):
        at = half * 256 + row
        fc = fine_ref[0, at : at + 16, j : j + 1]
        fs = fine_ref[1, at : at + 16, j : j + 1]
        bc = band_ref[0, row : row + 16, :]
        bs = band_ref[1, row : row + 16, :]
        c = (bc * fc - bs * fs).astype(bf16)
        s = (bs * fc + bc * fs).astype(bf16)
        if j % 2:
            wodd_ref[j // 2, at : at + 16, :] = c
            wodd_ref[j // 2, 512 + at : 512 + at + 16, :] = s
        else:
            weven_ref[j // 2, at : at + 16, :] = c
            weven_ref[j // 2, 256 + at : 256 + at + 16, :] = s

    def put(ref, index, row, col, depth, zr, zi):
        rh = zr.astype(bf16)
        ih = zi.astype(bf16)
        rl = (zr - rh.astype(f32)).astype(bf16)
        il = (zi - ih.astype(f32)).astype(bf16)
        for level, (re, im) in enumerate(((rh, ih), (rl, il))):
            ref[index, level, row : row + 16, col : col + 128] = re
            ref[index, level, row : row + 16, depth + col : depth + col + 128] = im
            ref[index, level, 256 + row : 256 + row + 16, col : col + 128] = im
            ref[index, level, 256 + row : 256 + row + 16, depth + col : depth + col + 128] = -re

    def quarters(g, part, cb):
        return [
            [
                x_ref[
                    g, c, part * 16 : part * 16 + 16, k * 512 + cb * 128 : k * 512 + cb * 128 + 128
                ].astype(f32)
                for k in range(4)
            ]
            for c in range(2)
        ]

    def fold_odd(g, part, cb):
        re, im = quarters(g, part, cb)
        dr, di = re[0] - re[2], im[0] - im[2]
        er, ei = re[1] - re[3], im[1] - im[3]
        row = g * ROWS + part * 16
        put(odd_ref, 0, row, cb * 128, 512, dr + ei, di - er)
        put(odd_ref, 1, row, cb * 128, 512, dr - ei, di + er)

    def fold_even(g, part, pair):
        row = g * ROWS + part * 16
        zs = []
        for cb in (pair, pair + 2):
            re, im = quarters(g, part, cb)
            sr, si = re[0] + re[2], im[0] + im[2]
            ur, ui = re[1] + re[3], im[1] + im[3]
            zs.append((sr + ur, si + ui, sr - ur, si - ui))
        (ar, ai, cr, ci), (br, bi, dr, di) = zs
        put(even_ref, 0, row, pair * 128, 256, ar + br, ai + bi)
        put(even_ref, 2, row, pair * 128, 256, ar - br, ai - bi)
        put(even_ref, 1, row, pair * 128, 256, cr + di, ci - dr)
        put(even_ref, 3, row, pair * 128, 256, cr - di, ci + dr)

    def walks_of():
        copies[1].wait()
        rows16 = iota((16, BANDS), 0) == (bands >> 4)
        walks = []
        for j in range(8):
            pick = iota((128, BANDS), 0) == (((bands & 15) << 3) + j)
            got = jnp.dot(
                walk_ref[...].astype(f32).astype(bf16),
                pick.astype(f32).astype(bf16),
                preferred_element_type=f32,
            )
            walk = jnp.sum(jnp.where(rows16, got, 0.0), axis=0, keepdims=True).astype(jnp.int32)
            own_ref[j : j + 1, :] = walk[:, 128:]
            walks.append(walk)
        return walks

    def align(j, tile):
        lanes = slice(tile * 128, tile * 128 + 128)
        walk = walks[j][:, lanes]
        ahead = walk >= 0
        at = [(walk * (8 * slow + g)) >> 6 for g in range(PER)]
        rim = jnp.zeros((WIN - ROWS, 128), f32)
        total = None
        for i in range(PER):
            own = jnp.where(
                ahead,
                power_ref[j, i * ROWS : (i + 1) * ROWS, lanes],
                power_ref[j, (7 - i) * ROWS : (8 - i) * ROWS, lanes],
            )
            own = jnp.concatenate([own, rim], axis=0)
            if i == 0:
                total = own
            else:
                step = jnp.where(ahead, at[i] - at[i - 1], at[7 - i] - at[8 - i]) == 1
                total = jnp.where(step, pltpu.roll(total, 1, 0), total) + own
        if tile == 0:
            send_ref[j] = total
            return
        keep_ref[j] = total
        lower = slow & ~1
        apart = jnp.where(
            ahead,
            ((walk * (8 * lower + 15)) >> 6) - ((walk * (8 * lower + 7)) >> 6),
            ((walk * (8 * lower)) >> 6) - ((walk * (8 * lower + 8)) >> 6),
        )
        meet_ref[j : j + 1, :] = jnp.where(ahead, apart, -apart - 1)

    def products(pair, count, at, side):
        depth = 1024 if pair[0] % 2 else 512
        sums = [None, None]
        for level in range(2):
            for k in range(0, depth, 256):
                for place, j in enumerate(pair):
                    if j % 2:
                        left, index, w = odd_ref, (j // 2) % 2, wodd_ref[j // 2, k : k + 256]
                    else:
                        left, index, w = even_ref, j // 2, weven_ref[j // 2, k : k + 256]
                    rows = jnp.concatenate(
                        [
                            left[index, level, at : at + count, k : k + 256],
                            left[index, level, 256 + at : 256 + at + count, k : k + 256],
                        ],
                        axis=0,
                    )
                    got = jnp.dot(rows, w, preferred_element_type=f32)
                    sums[place] = got if sums[place] is None else sums[place] + got
                share = -(-len(side) // (2 * depth // 256 - level * (depth // 256) - k // 256))
                for task in side[:share]:
                    task()
                side = side[share:]
        for place, j in enumerate(pair):
            re, im = sums[place][:count], sums[place][count:]
            power_ref[j, at : at + count, :] = re * re + im * im

    def later(task, *args):
        return lambda: task(*args)

    def folds(task, batches, cuts):
        return [later(task, g, p, c) for g in batches for p in range(2) for c in range(cuts)]

    def aligns(*bins):
        return [later(align, j, tile) for j in bins for tile in range(2)]

    def tables(*bins):
        return [
            later(table, j, half, row)
            for j in bins
            for half in range(2 if j % 2 else 1)
            for row in range(0, 256, 16)
        ]

    for task in tables(1, 5):
        task()
    walks = walks_of()
    for g in range(4):
        copies[2 + g].wait()
    for task in folds(fold_odd, range(4), 4):
        task()
    for g in range(4, 8):
        copies[2 + g].wait()
    products((1, 5), 128, 0, folds(fold_odd, range(4, 8), 4) + tables(3, 7))
    products((1, 5), 128, 128, folds(fold_even, range(4), 2) + tables(0, 4))
    products((3, 7), 256, 0, folds(fold_even, range(4, 8), 2) + tables(2, 6) + aligns(1, 5))
    products((0, 4), 256, 0, aligns(3, 7))
    products((2, 6), 256, 0, aligns(0, 4))
    for task in aligns(2, 6):
        task()


def pair_kernel(mine_ref, theirs_ref, meet_ref, out_ref, flat_ref):
    first = lax.axis_index("c") == 0
    for j in range(8):
        mine = mine_ref[j]
        theirs = theirs_ref[j]
        lower = jnp.where(first, mine, theirs)
        upper = jnp.where(first, theirs, mine)
        meet = meet_ref[j : j + 1, :]
        ahead = meet >= 0
        apart = jnp.where(ahead, meet, -meet - 1)
        moved = jnp.where(ahead, lower, upper)
        still = jnp.where(ahead, upper, lower)
        for bit in range(3):
            moved = jnp.where(((apart >> bit) & 1) == 1, pltpu.roll(moved, 1 << bit, 0), moved)
        flat_ref[j * WIN : (j + 1) * WIN, :] = moved + still
    flat_ref[8 * WIN :, :] = jnp.zeros((64, 128), f32)
    for piece in range(3):
        part = slice(piece * 128, (piece + 1) * 128)
        out_ref[:, part] = flat_ref[part, :].T


def join_kernel(walk_ref, x_ref, out_ref, turned_ref):
    lane = iota((1, 128), 1)
    group = lane // 32
    block = lane & 31
    here = lax.axis_index("x") * 32 + lax.axis_index("z") * 4 + lax.axis_index("y")
    walk = jnp.sum(jnp.where(lane == here, walk_ref[...], 0), axis=1, keepdims=True)
    batch = 16 * group + jnp.where(walk >= 0, 15, 0)
    moves = 32 - ((walk * batch) >> 6)
    flat = jnp.concatenate(
        [x_ref[:, piece * 128 : (piece + 1) * 128].T for piece in range(3)], axis=0
    )
    for quad in range(2):
        packed = None
        for jq in range(4):
            j = quad * 4 + jq
            move = moves[j : j + 1, :]
            current = jnp.concatenate(
                [flat[j * WIN : (j + 1) * WIN], jnp.zeros((8, 128), f32)], axis=0
            )
            for bit in range(6):
                taken = ((move >> bit) & 1) == 1
                if bit < 3:
                    current = jnp.where(taken, pltpu.roll(current, 1 << bit, 0), current)
                else:
                    pad = jnp.zeros((1 << bit, 128), f32)
                    low = jnp.concatenate([current, pad], axis=0)
                    high = jnp.concatenate([pad, current], axis=0)
                    current = jnp.where(taken, high[:96], low[:96])
            current = current + pltpu.roll(current, 64, 1)
            current = current + pltpu.roll(current, 32, 1)
            before = jnp.where(block == 31, 0.0, pltpu.roll(current[0:32], 127, 1))
            after = jnp.where(block == 0, 0.0, pltpu.roll(current[64:96], 1, 1))
            summed = before + current[32:64] + after
            packed = summed if packed is None else jnp.where(group == jq, summed, packed)
        packed = packed * SCALE
        turned_ref[quad * 128 : (quad + 1) * 128, :] = jnp.concatenate([packed] * 4, axis=0).T
    for v in range(8):
        result = None
        for c in range(4):
            piece = turned_ref[pl.ds(4 * v + c, 8, stride=32), :]
            result = piece if result is None else jnp.where(group == c, piece, result)
        out_ref[:, v * 128 : (v + 1) * 128] = result


VM = pl.BlockSpec(memory_space=pltpu.VMEM)


def on_device(profiles, range_walk, band_order):
    block = jax.ShapeDtypeStruct((8, WIN, 128), f32)
    row = jax.ShapeDtypeStruct((8, 128), jnp.int32)
    ANY = pl.BlockSpec(memory_space=pltpu.HBM)
    send, keep, meet, walks = pl.pallas_call(
        spectra_kernel,
        out_shape=(block, block, row, row),
        in_specs=[ANY, ANY, ANY],
        out_specs=(VM, VM, VM, VM),
        scratch_shapes=[
            pltpu.VMEM((PER, 2, ROWS, F), bf16),
            pltpu.VMEM((2, 128), jnp.int32),
            pltpu.VMEM((16, 128), jnp.int32),
            pltpu.VMEM((2, BANDS, BANDS), f32),
            pltpu.VMEM((2, 512, 128), f32),
            pltpu.VMEM((8, 256, 256), f32),
            pltpu.SemaphoreType.DMA((2 + PER,)),
        ],
        compiler_params=pltpu.CompilerParams(vmem_limit_bytes=GRANT),
    )(
        *(
            pltpu.with_memory_space_constraint(array, pltpu.HBM)
            for array in (profiles, band_order.reshape(2, 128), range_walk.reshape(16, 128))
        )
    )
    theirs = lax.ppermute(send, "c", [(0, 1), (1, 0)])
    messages = pl.pallas_call(
        pair_kernel,
        out_shape=jax.ShapeDtypeStruct((128, 384), f32),
        in_specs=[VM, VM, VM],
        out_specs=VM,
        scratch_shapes=[pltpu.VMEM((384, 128), f32)],
        compiler_params=pltpu.CompilerParams(vmem_limit_bytes=4 << 20),
    )(keep, theirs, meet)
    arrived = lax.all_to_all(
        messages.reshape(128, 1, 384), ("x", "z", "y"), split_axis=0, concat_axis=0, tiled=True
    )
    return pl.pallas_call(
        join_kernel,
        out_shape=jax.ShapeDtypeStruct((8, 1024), f32),
        in_specs=[VM, VM],
        out_specs=VM,
        scratch_shapes=[pltpu.VMEM((256, 128), f32)],
        compiler_params=pltpu.CompilerParams(vmem_limit_bytes=4 << 20),
    )(walks, arrived.reshape(128, 384))


def solution(mesh):
    fine = Mesh(mesh.devices.reshape(8, 4, 4, 2), ("z", "y", "x", "c"))
    placed = (P(("x", "c"), None, ("z", "y"), None), P(), P())
    return jax.shard_map(
        on_device, mesh=fine, in_specs=placed, out_specs=P(("z", "y", "x", "c"), None), check_vma=False
    )
```

```python
import math

import jax
import jax.numpy as jnp
from jax import lax
from jax.experimental import pallas as pl
from jax.experimental.pallas import tpu as pltpu
from jax.sharding import Mesh, PartitionSpec as P

F = 2048
BANDS = 256
ROWS = 32
PER = 8
WIN = 40
GRANT = 40 << 20
SCALE = 1.0 / (64 * F)
f32 = jnp.float32
bf16 = jnp.bfloat16


def cos_sin(turns, period):
    quarter = period // 4
    shift = quarter.bit_length() - 1
    quad = (turns + quarter // 2) >> shift
    r = (turns - (quad << shift)).astype(f32) * (2.0 * math.pi / period)
    r2 = r * r
    c = 1.0 + r2 * (-1 / 2 + r2 * (1 / 24 + r2 * (-1 / 720 + r2 * (1 / 40320))))
    s = r * (1.0 + r2 * (-1 / 6 + r2 * (1 / 120 + r2 * (-1 / 5040 + r2 * (1 / 362880)))))
    odd = (quad & 1) == 1
    cosine = jnp.where(odd, s, c)
    sine = jnp.where(odd, c, s)
    cosine = jnp.where(((quad + 1) & 2) == 2, -cosine, cosine)
    sine = jnp.where((quad & 2) == 2, -sine, sine)
    return cosine, sine


def iota(shape, dim):
    return lax.broadcasted_iota(jnp.int32, shape, dim)


def places():
    core = lax.axis_index("c")
    return 2 * lax.axis_index("x") + core, core


def spectra_kernel(
    x_hbm, order_hbm, walk_hbm, send_ref, keep_ref, meet_ref, own_ref,
    x_ref, order_ref, walk_ref, band_ref, fine_ref, power_ref, sems,
):
    copies = [
        pltpu.make_async_copy(order_hbm, order_ref, sems.at[0]),
        pltpu.make_async_copy(walk_hbm, walk_ref, sems.at[1]),
    ]
    copies += [
        pltpu.make_async_copy(x_hbm.at[g], x_ref.at[g], sems.at[2 + g]) for g in range(PER)
    ]
    for copy in copies:
        copy.start()
    packed = lambda *shape: pltpu.VMEM(shape, bf16)
    pl.run_scoped(
        lambda *refs: spectra(
            copies, send_ref, keep_ref, meet_ref, own_ref,
            x_ref, order_ref, walk_ref, band_ref, fine_ref, power_ref, *refs
        ),
        packed(2, 2, 512, 1024),
        packed(4, 2, 512, 512),
        packed(4, 1024, 256),
        packed(4, 512, 256),
    )


def spectra(
    copies, send_ref, keep_ref, meet_ref, own_ref,
    x_ref, order_ref, walk_ref, band_ref, fine_ref, power_ref,
    odd_ref, even_ref, wodd_ref, weven_ref,
):
    slow, core = places()
    zero = slow >> 8
    fine = cos_sin((iota((8, 512), 1) * iota((8, 512), 0)) & (F - 1), F)
    blank = jnp.zeros((120, 128), f32)
    for part in range(2):
        for at in range(0, 512, 128):
            fine_ref[part, at : at + 128, :] = jnp.concatenate(
                [fine[part][:, at : at + 128], blank], axis=0
            ).T

    copies[0].wait()
    order = order_ref[...].astype(f32).astype(bf16)
    halves = []
    for c in range(2):
        owner = ((iota((128, 128), 1) & 31) << 3) + ((iota((128, 128), 1) >> 5) << 1) + c
        pick = iota((128, 128), 0) == (owner & 127)
        got = jnp.dot(order, pick.astype(f32).astype(bf16), preferred_element_type=f32)
        halves.append(jnp.where((iota((1, 128), 1) & 31) < 16, got[0:1], got[1:2]))
    flip = core == 0
    bands = jnp.concatenate(
        [jnp.where(flip, halves[1], halves[0]), jnp.where(flip, halves[0], halves[1])], axis=1
    ).astype(jnp.int32)

    steps = [(bands * k) & 3 for k in range(4)]
    real = [jnp.where(k == 0, 1.0, jnp.where(k == 2, -1.0, 0.0)) for k in steps]
    imag = [jnp.where(k == 1, 1.0, jnp.where(k == 3, -1.0, 0.0)) for k in steps]
    for at in range(0, 64, 16):
        c, s = cos_sin(((iota((16, BANDS), 0) + at) * bands) & (BANDS - 1), BANDS)
        band_ref[0, at : at + 16, :] = c
        band_ref[1, at : at + 16, :] = s
        for k in range(1, 4):
            band_ref[0, k * 64 + at : k * 64 + at + 16, :] = c * real[k] - s * imag[k]
            band_ref[1, k * 64 + at : k * 64 + at + 16, :] = s * real[k] + c * imag[k]

    def table(j, half, row):
        at = half * 256 + row
        fc = fine_ref[0 + zero, at : at + 16, j : j + 1]
        fs = fine_ref[1 + zero, at : at + 16, j : j + 1]
        bc = band_ref[0 + zero, row : row + 16, :]
        bs = band_ref[1 + zero, row : row + 16, :]
        c = (bc * fc - bs * fs).astype(bf16)
        s = (bs * fc + bc * fs).astype(bf16)
        if j % 2:
            wodd_ref[j // 2, at : at + 16, :] = c
            wodd_ref[j // 2, 512 + at : 512 + at + 16, :] = s
        else:
            weven_ref[j // 2, at : at + 16, :] = c
            weven_ref[j // 2, 256 + at : 256 + at + 16, :] = s

    def put(ref, index, row, col, depth, zr, zi):
        rh = zr.astype(bf16)
        ih = zi.astype(bf16)
        rl = (zr - rh.astype(f32)).astype(bf16)
        il = (zi - ih.astype(f32)).astype(bf16)
        for level, (re, im) in enumerate(((rh, ih), (rl, il))):
            ref[index, level, row : row + 16, col : col + 128] = re
            ref[index, level, row : row + 16, depth + col : depth + col + 128] = im
            ref[index, level, 256 + row : 256 + row + 16, col : col + 128] = im
            ref[index, level, 256 + row : 256 + row + 16, depth + col : depth + col + 128] = -re

    def quarters(g, part, cb):
        return [
            [
                x_ref[
                    g, c, part * 16 : part * 16 + 16, k * 512 + cb * 128 : k * 512 + cb * 128 + 128
                ].astype(f32)
                for k in range(4)
            ]
            for c in range(2)
        ]

    def fold_odd(g, part, cb):
        re, im = quarters(g, part, cb)
        dr, di = re[0] - re[2], im[0] - im[2]
        er, ei = re[1] - re[3], im[1] - im[3]
        row = g * ROWS + part * 16
        put(odd_ref, 0, row, cb * 128, 512, dr + ei, di - er)
        put(odd_ref, 1, row, cb * 128, 512, dr - ei, di + er)

    def fold_even(g, part, pair):
        row = g * ROWS + part * 16
        zs = []
        for cb in (pair, pair + 2):
            re, im = quarters(g, part, cb)
            sr, si = re[0] + re[2], im[0] + im[2]
            ur, ui = re[1] + re[3], im[1] + im[3]
            zs.append((sr + ur, si + ui, sr - ur, si - ui))
        (ar, ai, cr, ci), (br, bi, dr, di) = zs
        put(even_ref, 0, row, pair * 128, 256, ar + br, ai + bi)
        put(even_ref, 2, row, pair * 128, 256, ar - br, ai - bi)
        put(even_ref, 1, row, pair * 128, 256, cr + di, ci - dr)
        put(even_ref, 3, row, pair * 128, 256, cr - di, ci + dr)

    def walks_of():
        copies[1].wait()
        rows16 = iota((16, BANDS), 0) == (bands >> 4)
        pick = iota((128, BANDS), 0) == ((bands & 15) << 3)
        held = walk_ref[...].astype(f32)
        shifts = jnp.concatenate(
            [held if j == 0 else pltpu.roll(held, 128 - j, 1) for j in range(8)], axis=0
        )
        got = jnp.dot(
            shifts.astype(bf16), pick.astype(f32).astype(bf16), preferred_element_type=f32
        )
        walks = []
        for j in range(8):
            mine = jnp.where(rows16, got[j * 16 : j * 16 + 16], 0.0)
            walk = jnp.sum(mine, axis=0, keepdims=True).astype(jnp.int32)
            own_ref[j : j + 1, :] = walk[:, 128:]
            walks.append(walk)
        return walks

    def align(j, tile):
        lanes = slice(tile * 128, tile * 128 + 128)
        walk = walks[j][:, lanes]
        ahead = walk >= 0
        at = [(walk * (8 * slow + g)) >> 6 for g in range(PER)]
        rim = jnp.zeros((WIN - ROWS, 128), f32)
        total = None
        for i in range(PER):
            own = jnp.where(
                ahead,
                power_ref[j + zero, i * ROWS : (i + 1) * ROWS, lanes],
                power_ref[j + zero, (7 - i) * ROWS : (8 - i) * ROWS, lanes],
            )
            own = jnp.concatenate([own, rim], axis=0)
            if i == 0:
                total = own
            else:
                step = jnp.where(ahead, at[i] - at[i - 1], at[7 - i] - at[8 - i]) == 1
                total = jnp.where(step, pltpu.roll(total, 1, 0), total) + own
        if tile == 0:
            send_ref[j] = total
            return
        keep_ref[j] = total
        lower = slow & ~1
        apart = jnp.where(
            ahead,
            ((walk * (8 * lower + 15)) >> 6) - ((walk * (8 * lower + 7)) >> 6),
            ((walk * (8 * lower)) >> 6) - ((walk * (8 * lower + 8)) >> 6),
        )
        meet_ref[j : j + 1, :] = jnp.where(ahead, apart, -apart - 1)

    def products(pair, count, at, side):
        depth = 1024 if pair[0] % 2 else 512
        sums = [None, None]
        for level in range(2):
            for k in range(0, depth, 256):
                for place, j in enumerate(pair):
                    if j % 2:
                        left, index, w = odd_ref, (j // 2) % 2 + zero, wodd_ref[j // 2 + zero, k : k + 256]
                    else:
                        left, index, w = even_ref, j // 2 + zero, weven_ref[j // 2 + zero, k : k + 256]
                    rows = jnp.concatenate(
                        [
                            left[index, level, at : at + count, k : k + 256],
                            left[index, level, 256 + at : 256 + at + count, k : k + 256],
                        ],
                        axis=0,
                    )
                    got = jnp.dot(rows, w, preferred_element_type=f32)
                    sums[place] = got if sums[place] is None else sums[place] + got
                share = -(-len(side) // (2 * depth // 256 - level * (depth // 256) - k // 256))
                for task in side[:share]:
                    task()
                side = side[share:]
        for place, j in enumerate(pair):
            re, im = sums[place][:count], sums[place][count:]
            power_ref[j, at : at + count, :] = re * re + im * im

    def later(task, *args):
        return lambda: task(*args)

    def folds(task, batches, cuts):
        return [later(task, g, p, c) for g in batches for p in range(2) for c in range(cuts)]

    def aligns(*bins):
        return [later(align, j, tile) for j in bins for tile in range(2)]

    def tables(*bins):
        return [
            later(table, j, half, row)
            for j in bins
            for half in range(2 if j % 2 else 1)
            for row in range(0, 256, 16)
        ]

    for task in tables(1, 5):
        task()
    walks = walks_of()
    for g in range(4):
        copies[2 + g].wait()
    for task in folds(fold_odd, range(4), 4):
        task()
    for g in range(4, 8):
        copies[2 + g].wait()
    products((1, 5), 128, 0, folds(fold_odd, range(4, 8), 4) + tables(3, 7))
    products((1, 5), 128, 128, folds(fold_even, range(4), 2))
    products((3, 7), 256, 0, folds(fold_even, range(4, 8), 2) + tables(0, 4, 2, 6) + aligns(1, 5))

    @pl.when(zero == 0)
    def evens():
        products((0, 4), 256, 0, aligns(3, 7))
        products((2, 6), 256, 0, aligns(0, 4))
        for task in aligns(2, 6):
            task()


def pair_kernel(mine_ref, theirs_ref, meet_ref, out_ref, flat_ref):
    first = lax.axis_index("c") == 0
    for j in range(8):
        mine = mine_ref[j]
        theirs = theirs_ref[j]
        lower = jnp.where(first, mine, theirs)
        upper = jnp.where(first, theirs, mine)
        meet = meet_ref[j : j + 1, :]
        ahead = meet >= 0
        apart = jnp.where(ahead, meet, -meet - 1)
        moved = jnp.where(ahead, lower, upper)
        still = jnp.where(ahead, upper, lower)
        for bit in range(3):
            moved = jnp.where(((apart >> bit) & 1) == 1, pltpu.roll(moved, 1 << bit, 0), moved)
        flat_ref[j * WIN : (j + 1) * WIN, :] = moved + still
    flat_ref[8 * WIN :, :] = jnp.zeros((64, 128), f32)
    for piece in range(3):
        part = slice(piece * 128, (piece + 1) * 128)
        out_ref[:, part] = flat_ref[part, :].T


def join_kernel(walk_ref, x_ref, out_ref, turned_ref):
    lane = iota((1, 128), 1)
    group = lane // 32
    block = lane & 31
    here = lax.axis_index("x") * 32 + lax.axis_index("z") * 4 + lax.axis_index("y")
    walk = jnp.sum(jnp.where(lane == here, walk_ref[...], 0), axis=1, keepdims=True)
    batch = 16 * group + jnp.where(walk >= 0, 15, 0)
    moves = 32 - ((walk * batch) >> 6)
    flat = jnp.concatenate(
        [x_ref[:, piece * 128 : (piece + 1) * 128].T for piece in range(3)], axis=0
    )
    for quad in range(2):
        packed = None
        for jq in range(4):
            j = quad * 4 + jq
            move = moves[j : j + 1, :]
            current = jnp.concatenate(
                [flat[j * WIN : (j + 1) * WIN], jnp.zeros((8, 128), f32)], axis=0
            )
            for bit in range(6):
                taken = ((move >> bit) & 1) == 1
                if bit < 3:
                    current = jnp.where(taken, pltpu.roll(current, 1 << bit, 0), current)
                else:
                    pad = jnp.zeros((1 << bit, 128), f32)
                    low = jnp.concatenate([current, pad], axis=0)
                    high = jnp.concatenate([pad, current], axis=0)
                    current = jnp.where(taken, high[:96], low[:96])
            current = current + pltpu.roll(current, 64, 1)
            current = current + pltpu.roll(current, 32, 1)
            before = jnp.where(block == 31, 0.0, pltpu.roll(current[0:32], 127, 1))
            after = jnp.where(block == 0, 0.0, pltpu.roll(current[64:96], 1, 1))
            summed = before + current[32:64] + after
            packed = summed if packed is None else jnp.where(group == jq, summed, packed)
        packed = packed * SCALE
        turned_ref[quad * 128 : (quad + 1) * 128, :] = jnp.concatenate([packed] * 4, axis=0).T
    for v in range(8):
        result = None
        for c in range(4):
            piece = turned_ref[pl.ds(4 * v + c, 8, stride=32), :]
            result = piece if result is None else jnp.where(group == c, piece, result)
        out_ref[:, v * 128 : (v + 1) * 128] = result


VM = pl.BlockSpec(memory_space=pltpu.VMEM)


def on_device(profiles, range_walk, band_order):
    block = jax.ShapeDtypeStruct((8, WIN, 128), f32)
    row = jax.ShapeDtypeStruct((8, 128), jnp.int32)
    ANY = pl.BlockSpec(memory_space=pltpu.HBM)
    send, keep, meet, walks = pl.pallas_call(
        spectra_kernel,
        out_shape=(block, block, row, row),
        in_specs=[ANY, ANY, ANY],
        out_specs=(VM, VM, VM, VM),
        scratch_shapes=[
            pltpu.VMEM((PER, 2, ROWS, F), bf16),
            pltpu.VMEM((2, 128), jnp.int32),
            pltpu.VMEM((16, 128), jnp.int32),
            pltpu.VMEM((2, BANDS, BANDS), f32),
            pltpu.VMEM((2, 512, 128), f32),
            pltpu.VMEM((8, 256, 256), f32),
            pltpu.SemaphoreType.DMA((2 + PER,)),
        ],
        compiler_params=pltpu.CompilerParams(vmem_limit_bytes=GRANT),
    )(
        *(
            pltpu.with_memory_space_constraint(array, pltpu.HBM)
            for array in (profiles, band_order.reshape(2, 128), range_walk.reshape(16, 128))
        )
    )
    theirs = lax.ppermute(send, "c", [(0, 1), (1, 0)])
    messages = pl.pallas_call(
        pair_kernel,
        out_shape=jax.ShapeDtypeStruct((128, 384), f32),
        in_specs=[VM, VM, VM],
        out_specs=VM,
        scratch_shapes=[pltpu.VMEM((384, 128), f32)],
        compiler_params=pltpu.CompilerParams(vmem_limit_bytes=4 << 20),
    )(keep, theirs, meet)
    arrived = lax.all_to_all(
        messages.reshape(128, 1, 384), ("x", "z", "y"), split_axis=0, concat_axis=0, tiled=True
    )
    return pl.pallas_call(
        join_kernel,
        out_shape=jax.ShapeDtypeStruct((8, 1024), f32),
        in_specs=[VM, VM],
        out_specs=VM,
        scratch_shapes=[pltpu.VMEM((256, 128), f32)],
        compiler_params=pltpu.CompilerParams(vmem_limit_bytes=4 << 20),
    )(walks, arrived.reshape(128, 384))


def solution(mesh):
    fine = Mesh(mesh.devices.reshape(8, 4, 4, 2), ("z", "y", "x", "c"))
    placed = (P(("x", "c"), None, ("z", "y"), None), P(), P())
    return jax.shard_map(
        on_device, mesh=fine, in_specs=placed, out_specs=P(("z", "y", "x", "c"), None), check_vma=False
    )
```

```python
import math

import jax
import jax.numpy as jnp
from jax import lax
from jax.experimental import pallas as pl
from jax.experimental.pallas import tpu as pltpu
from jax.sharding import Mesh, PartitionSpec as P

F = 2048
BANDS = 256
ROWS = 32
PER = 8
WIN = 40
GRANT = 40 << 20
SCALE = 1.0 / (64 * F)
f32 = jnp.float32
bf16 = jnp.bfloat16


def cos_sin(turns, period):
    quarter = period // 4
    shift = quarter.bit_length() - 1
    quad = (turns + quarter // 2) >> shift
    r = (turns - (quad << shift)).astype(f32) * (2.0 * math.pi / period)
    r2 = r * r
    c = 1.0 + r2 * (-1 / 2 + r2 * (1 / 24 + r2 * (-1 / 720 + r2 * (1 / 40320))))
    s = r * (1.0 + r2 * (-1 / 6 + r2 * (1 / 120 + r2 * (-1 / 5040 + r2 * (1 / 362880)))))
    odd = (quad & 1) == 1
    cosine = jnp.where(odd, s, c)
    sine = jnp.where(odd, c, s)
    cosine = jnp.where(((quad + 1) & 2) == 2, -cosine, cosine)
    sine = jnp.where((quad & 2) == 2, -sine, sine)
    return cosine, sine


def iota(shape, dim):
    return lax.broadcasted_iota(jnp.int32, shape, dim)


def places():
    core = lax.axis_index("c")
    return 2 * lax.axis_index("x") + core, core


def spectra_kernel(
    x_hbm, order_hbm, walk_hbm, send_ref, keep_ref, meet_ref, own_ref,
    x_ref, order_ref, walk_ref, band_ref, fine_ref, power_ref, sems,
):
    copies = [
        pltpu.make_async_copy(order_hbm, order_ref, sems.at[0]),
        pltpu.make_async_copy(walk_hbm, walk_ref, sems.at[1]),
    ]
    copies += [
        pltpu.make_async_copy(x_hbm.at[g], x_ref.at[g], sems.at[2 + g]) for g in range(PER)
    ]
    for copy in copies:
        copy.start()
    packed = lambda *shape: pltpu.VMEM(shape, bf16)
    pl.run_scoped(
        lambda *refs: spectra(
            copies, send_ref, keep_ref, meet_ref, own_ref,
            x_ref, order_ref, walk_ref, band_ref, fine_ref, power_ref, *refs
        ),
        packed(2, 2, 512, 1024),
        packed(4, 2, 512, 512),
        packed(4, 1024, 256),
        packed(4, 512, 256),
    )


def spectra(
    copies, send_ref, keep_ref, meet_ref, own_ref,
    x_ref, order_ref, walk_ref, band_ref, fine_ref, power_ref,
    odd_ref, even_ref, wodd_ref, weven_ref,
):
    slow, core = places()
    zero = slow >> 8
    fine = cos_sin((iota((8, 512), 1) * iota((8, 512), 0)) & (F - 1), F)
    blank = jnp.zeros((120, 128), f32)
    for part in range(2):
        for at in range(0, 512, 128):
            fine_ref[part, at : at + 128, :] = jnp.concatenate(
                [fine[part][:, at : at + 128], blank], axis=0
            ).T

    copies[0].wait()
    order = order_ref[...].astype(f32).astype(bf16)
    halves = []
    for c in range(2):
        owner = ((iota((128, 128), 1) & 31) << 3) + ((iota((128, 128), 1) >> 5) << 1) + c
        pick = iota((128, 128), 0) == (owner & 127)
        got = jnp.dot(order, pick.astype(f32).astype(bf16), preferred_element_type=f32)
        halves.append(jnp.where((iota((1, 128), 1) & 31) < 16, got[0:1], got[1:2]))
    flip = core == 0
    bands = jnp.concatenate(
        [jnp.where(flip, halves[1], halves[0]), jnp.where(flip, halves[0], halves[1])], axis=1
    ).astype(jnp.int32)

    steps = [(bands * k) & 3 for k in range(4)]
    real = [jnp.where(k == 0, 1.0, jnp.where(k == 2, -1.0, 0.0)) for k in steps]
    imag = [jnp.where(k == 1, 1.0, jnp.where(k == 3, -1.0, 0.0)) for k in steps]
    for at in range(0, 64, 16):
        c, s = cos_sin(((iota((16, BANDS), 0) + at) * bands) & (BANDS - 1), BANDS)
        band_ref[0, at : at + 16, :] = c
        band_ref[1, at : at + 16, :] = s
        for k in range(1, 4):
            band_ref[0, k * 64 + at : k * 64 + at + 16, :] = c * real[k] - s * imag[k]
            band_ref[1, k * 64 + at : k * 64 + at + 16, :] = s * real[k] + c * imag[k]

    def table(j, half, row):
        at = half * 256 + row
        fc = fine_ref[0, at : at + 16, j : j + 1]
        fs = fine_ref[1, at : at + 16, j : j + 1]
        bc = band_ref[0, row : row + 16, :]
        bs = band_ref[1, row : row + 16, :]
        c = (bc * fc - bs * fs).astype(bf16)
        s = (bs * fc + bc * fs).astype(bf16)
        if j % 2:
            wodd_ref[j // 2, at : at + 16, :] = c
            wodd_ref[j // 2, 512 + at : 512 + at + 16, :] = s
        else:
            weven_ref[j // 2, at : at + 16, :] = c
            weven_ref[j // 2, 256 + at : 256 + at + 16, :] = s

    def put(ref, index, row, col, depth, zr, zi):
        rh = zr.astype(bf16)
        ih = zi.astype(bf16)
        rl = (zr - rh.astype(f32)).astype(bf16)
        il = (zi - ih.astype(f32)).astype(bf16)
        for level, (re, im) in enumerate(((rh, ih), (rl, il))):
            ref[index, level, row : row + 16, col : col + 128] = re
            ref[index, level, row : row + 16, depth + col : depth + col + 128] = im
            ref[index, level, 256 + row : 256 + row + 16, col : col + 128] = im
            ref[index, level, 256 + row : 256 + row + 16, depth + col : depth + col + 128] = -re

    def quarters(g, part, cb):
        return [
            [
                x_ref[
                    g, c, part * 16 : part * 16 + 16, k * 512 + cb * 128 : k * 512 + cb * 128 + 128
                ].astype(f32)
                for k in range(4)
            ]
            for c in range(2)
        ]

    def fold_odd(g, part, cb):
        re, im = quarters(g, part, cb)
        dr, di = re[0] - re[2], im[0] - im[2]
        er, ei = re[1] - re[3], im[1] - im[3]
        row = g * ROWS + part * 16
        put(odd_ref, 0, row, cb * 128, 512, dr + ei, di - er)
        put(odd_ref, 1, row, cb * 128, 512, dr - ei, di + er)

    def fold_even(g, part, pair):
        row = g * ROWS + part * 16
        zs = []
        for cb in (pair, pair + 2):
            re, im = quarters(g, part, cb)
            sr, si = re[0] + re[2], im[0] + im[2]
            ur, ui = re[1] + re[3], im[1] + im[3]
            zs.append((sr + ur, si + ui, sr - ur, si - ui))
        (ar, ai, cr, ci), (br, bi, dr, di) = zs
        put(even_ref, 0, row, pair * 128, 256, ar + br, ai + bi)
        put(even_ref, 2, row, pair * 128, 256, ar - br, ai - bi)
        put(even_ref, 1, row, pair * 128, 256, cr + di, ci - dr)
        put(even_ref, 3, row, pair * 128, 256, cr - di, ci + dr)

    def walks_of():
        copies[1].wait()
        rows16 = iota((16, BANDS), 0) == (bands >> 4)
        pick = iota((128, BANDS), 0) == ((bands & 15) << 3)
        held = walk_ref[...].astype(f32)
        shifts = jnp.concatenate(
            [held if j == 0 else pltpu.roll(held, 128 - j, 1) for j in range(8)], axis=0
        )
        got = jnp.dot(
            shifts.astype(bf16), pick.astype(f32).astype(bf16), preferred_element_type=f32
        )
        walks = []
        for j in range(8):
            mine = jnp.where(rows16, got[j * 16 : j * 16 + 16], 0.0)
            walk = jnp.sum(mine, axis=0, keepdims=True).astype(jnp.int32)
            own_ref[j : j + 1, :] = walk[:, 128:]
            walks.append(walk)
        return walks

    def align(j, tile):
        lanes = slice(tile * 128, tile * 128 + 128)
        walk = walks[j][:, lanes]
        ahead = walk >= 0
        at = [(walk * (8 * slow + g)) >> 6 for g in range(PER)]
        rim = jnp.zeros((WIN - ROWS, 128), f32)
        total = None
        for i in range(PER):
            own = jnp.where(
                ahead,
                power_ref[j, i * ROWS : (i + 1) * ROWS, lanes],
                power_ref[j, (7 - i) * ROWS : (8 - i) * ROWS, lanes],
            )
            own = jnp.concatenate([own, rim], axis=0)
            if i == 0:
                total = own
            else:
                step = jnp.where(ahead, at[i] - at[i - 1], at[7 - i] - at[8 - i]) == 1
                total = jnp.where(step, pltpu.roll(total, 1, 0), total) + own
        if tile == 0:
            send_ref[j] = total
            return
        keep_ref[j] = total
        lower = slow & ~1
        apart = jnp.where(
            ahead,
            ((walk * (8 * lower + 15)) >> 6) - ((walk * (8 * lower + 7)) >> 6),
            ((walk * (8 * lower)) >> 6) - ((walk * (8 * lower + 8)) >> 6),
        )
        meet_ref[j : j + 1, :] = jnp.where(ahead, apart, -apart - 1)

    def products(pair, count, at, side):
        depth = 1024 if pair[0] % 2 else 512
        sums = [None, None]
        for level in range(2):
            for k in range(0, depth, 256):
                for place, j in enumerate(pair):
                    if j % 2:
                        left, index, w = odd_ref, (j // 2) % 2, wodd_ref[j // 2, k : k + 256]
                    else:
                        left, index, w = even_ref, j // 2, weven_ref[j // 2, k : k + 256]
                    rows = jnp.concatenate(
                        [
                            left[index, level, at : at + count, k : k + 256],
                            left[index, level, 256 + at : 256 + at + count, k : k + 256],
                        ],
                        axis=0,
                    )
                    got = jnp.dot(rows, w, preferred_element_type=f32)
                    sums[place] = got if sums[place] is None else sums[place] + got
                share = -(-len(side) // (2 * depth // 256 - level * (depth // 256) - k // 256))
                for task in side[:share]:
                    task()
                side = side[share:]
        for place, j in enumerate(pair):
            re, im = sums[place][:count], sums[place][count:]
            power_ref[j, at : at + count, :] = re * re + im * im

    def later(task, *args):
        return lambda: task(*args)

    def folds(task, batches, cuts):
        return [later(task, g, p, c) for g in batches for p in range(2) for c in range(cuts)]

    def aligns(*bins):
        return [later(align, j, tile) for j in bins for tile in range(2)]

    def tables(*bins):
        return [
            later(table, j, half, row)
            for j in bins
            for half in range(2 if j % 2 else 1)
            for row in range(0, 256, 16)
        ]

    for task in tables(1, 5):
        task()
    walks = walks_of()
    for g in range(4):
        copies[2 + g].wait()
    for task in folds(fold_odd, range(4), 4):
        task()
    for g in range(4, 8):
        copies[2 + g].wait()
    products((1, 5), 128, 0, folds(fold_odd, range(4, 8), 4) + tables(3, 7))
    products((1, 5), 128, 128, folds(fold_even, range(8), 2))
    products((3, 7), 256, 0, tables(0, 4, 2, 6) + aligns(1, 5))
    products((0, 4), 256, 0, aligns(3, 7))
    products((2, 6), 256, 0, aligns(0, 4))
    for task in aligns(2, 6):
        task()


def pair_kernel(mine_ref, theirs_ref, meet_ref, out_ref, flat_ref):
    first = lax.axis_index("c") == 0
    for j in range(8):
        mine = mine_ref[j]
        theirs = theirs_ref[j]
        lower = jnp.where(first, mine, theirs)
        upper = jnp.where(first, theirs, mine)
        meet = meet_ref[j : j + 1, :]
        ahead = meet >= 0
        apart = jnp.where(ahead, meet, -meet - 1)
        moved = jnp.where(ahead, lower, upper)
        still = jnp.where(ahead, upper, lower)
        for bit in range(3):
            moved = jnp.where(((apart >> bit) & 1) == 1, pltpu.roll(moved, 1 << bit, 0), moved)
        flat_ref[j * WIN : (j + 1) * WIN, :] = moved + still
    flat_ref[8 * WIN :, :] = jnp.zeros((64, 128), f32)
    for piece in range(3):
        part = slice(piece * 128, (piece + 1) * 128)
        out_ref[:, part] = flat_ref[part, :].T


def join_kernel(walk_ref, x_ref, out_ref, turned_ref):
    lane = iota((1, 128), 1)
    group = lane // 32
    block = lane & 31
    here = lax.axis_index("x") * 32 + lax.axis_index("z") * 4 + lax.axis_index("y")
    walk = jnp.sum(jnp.where(lane == here, walk_ref[...], 0), axis=1, keepdims=True)
    batch = 16 * group + jnp.where(walk >= 0, 15, 0)
    moves = 32 - ((walk * batch) >> 6)
    flat = jnp.concatenate(
        [x_ref[:, piece * 128 : (piece + 1) * 128].T for piece in range(3)], axis=0
    )
    for quad in range(2):
        packed = None
        for jq in range(4):
            j = quad * 4 + jq
            move = moves[j : j + 1, :]
            current = jnp.concatenate(
                [flat[j * WIN : (j + 1) * WIN], jnp.zeros((8, 128), f32)], axis=0
            )
            for bit in range(6):
                taken = ((move >> bit) & 1) == 1
                if bit < 3:
                    current = jnp.where(taken, pltpu.roll(current, 1 << bit, 0), current)
                else:
                    pad = jnp.zeros((1 << bit, 128), f32)
                    low = jnp.concatenate([current, pad], axis=0)
                    high = jnp.concatenate([pad, current], axis=0)
                    current = jnp.where(taken, high[:96], low[:96])
            current = current + pltpu.roll(current, 64, 1)
            current = current + pltpu.roll(current, 32, 1)
            before = jnp.where(block == 31, 0.0, pltpu.roll(current[0:32], 127, 1))
            after = jnp.where(block == 0, 0.0, pltpu.roll(current[64:96], 1, 1))
            summed = before + current[32:64] + after
            packed = summed if packed is None else jnp.where(group == jq, summed, packed)
        packed = packed * SCALE
        turned_ref[quad * 128 : (quad + 1) * 128, :] = jnp.concatenate([packed] * 4, axis=0).T
    for v in range(8):
        result = None
        for c in range(4):
            piece = turned_ref[pl.ds(4 * v + c, 8, stride=32), :]
            result = piece if result is None else jnp.where(group == c, piece, result)
        out_ref[:, v * 128 : (v + 1) * 128] = result


VM = pl.BlockSpec(memory_space=pltpu.VMEM)


def on_device(profiles, range_walk, band_order):
    block = jax.ShapeDtypeStruct((8, WIN, 128), f32)
    row = jax.ShapeDtypeStruct((8, 128), jnp.int32)
    ANY = pl.BlockSpec(memory_space=pltpu.HBM)
    send, keep, meet, walks = pl.pallas_call(
        spectra_kernel,
        out_shape=(block, block, row, row),
        in_specs=[ANY, ANY, ANY],
        out_specs=(VM, VM, VM, VM),
        scratch_shapes=[
            pltpu.VMEM((PER, 2, ROWS, F), bf16),
            pltpu.VMEM((2, 128), jnp.int32),
            pltpu.VMEM((16, 128), jnp.int32),
            pltpu.VMEM((2, BANDS, BANDS), f32),
            pltpu.VMEM((2, 512, 128), f32),
            pltpu.VMEM((8, 256, 256), f32),
            pltpu.SemaphoreType.DMA((2 + PER,)),
        ],
        compiler_params=pltpu.CompilerParams(vmem_limit_bytes=GRANT),
    )(
        *(
            pltpu.with_memory_space_constraint(array, pltpu.HBM)
            for array in (profiles, band_order.reshape(2, 128), range_walk.reshape(16, 128))
        )
    )
    theirs = lax.ppermute(send, "c", [(0, 1), (1, 0)])
    messages = pl.pallas_call(
        pair_kernel,
        out_shape=jax.ShapeDtypeStruct((128, 384), f32),
        in_specs=[VM, VM, VM],
        out_specs=VM,
        scratch_shapes=[pltpu.VMEM((384, 128), f32)],
        compiler_params=pltpu.CompilerParams(vmem_limit_bytes=4 << 20),
    )(keep, theirs, meet)
    arrived = lax.all_to_all(
        messages.reshape(128, 1, 384), ("x", "z", "y"), split_axis=0, concat_axis=0, tiled=True
    )
    return pl.pallas_call(
        join_kernel,
        out_shape=jax.ShapeDtypeStruct((8, 1024), f32),
        in_specs=[VM, VM],
        out_specs=VM,
        scratch_shapes=[pltpu.VMEM((256, 128), f32)],
        compiler_params=pltpu.CompilerParams(vmem_limit_bytes=4 << 20),
    )(walks, arrived.reshape(128, 384))


def solution(mesh):
    fine = Mesh(mesh.devices.reshape(8, 4, 4, 2), ("z", "y", "x", "c"))
    placed = (P(("x", "c"), None, ("z", "y"), None), P(), P())
    return jax.shard_map(
        on_device, mesh=fine, in_specs=placed, out_specs=P(("z", "y", "x", "c"), None), check_vma=False
    )
```

```python
import math

import jax
import jax.numpy as jnp
from jax import lax
from jax.experimental import pallas as pl
from jax.experimental.pallas import tpu as pltpu
from jax.sharding import Mesh, PartitionSpec as P

F = 2048
BANDS = 256
ROWS = 32
PER = 8
WIN = 40
HALF_ROOT = math.sqrt(0.5)
GRANT = 40 << 20
SCALE = 1.0 / (64 * F)
f32 = jnp.float32
bf16 = jnp.bfloat16


def cos_sin(turns, period):
    quarter = period // 4
    shift = quarter.bit_length() - 1
    quad = (turns + quarter // 2) >> shift
    r = (turns - (quad << shift)).astype(f32) * (2.0 * math.pi / period)
    r2 = r * r
    c = 1.0 + r2 * (-1 / 2 + r2 * (1 / 24 + r2 * (-1 / 720 + r2 * (1 / 40320))))
    s = r * (1.0 + r2 * (-1 / 6 + r2 * (1 / 120 + r2 * (-1 / 5040 + r2 * (1 / 362880)))))
    odd = (quad & 1) == 1
    cosine = jnp.where(odd, s, c)
    sine = jnp.where(odd, c, s)
    cosine = jnp.where(((quad + 1) & 2) == 2, -cosine, cosine)
    sine = jnp.where((quad & 2) == 2, -sine, sine)
    return cosine, sine


def iota(shape, dim):
    return lax.broadcasted_iota(jnp.int32, shape, dim)


def places():
    core = lax.axis_index("c")
    return 2 * lax.axis_index("x") + core, core


def spectra_kernel(
    x_hbm, order_hbm, walk_hbm, send_ref, keep_ref, meet_ref, own_ref,
    x_ref, order_ref, walk_ref, band_ref, fine_ref, power_ref, sems,
):
    copies = [
        pltpu.make_async_copy(order_hbm, order_ref, sems.at[0]),
        pltpu.make_async_copy(walk_hbm, walk_ref, sems.at[1]),
    ]
    copies += [
        pltpu.make_async_copy(x_hbm.at[g], x_ref.at[g], sems.at[2 + g]) for g in range(PER)
    ]
    for copy in copies:
        copy.start()
    packed = lambda *shape: pltpu.VMEM(shape, bf16)
    pl.run_scoped(
        lambda *refs: spectra(
            copies, send_ref, keep_ref, meet_ref, own_ref,
            x_ref, order_ref, walk_ref, band_ref, fine_ref, power_ref, *refs
        ),
        packed(2, 512, 1024),
        packed(4, 512, 512),
        packed(8, 512, 512),
        packed(4, 1024, 256),
        packed(4, 512, 256),
    )


def spectra(
    copies, send_ref, keep_ref, meet_ref, own_ref,
    x_ref, order_ref, walk_ref, band_ref, fine_ref, power_ref,
    odd_ref, even_ref, low_ref, wodd_ref, weven_ref,
):
    slow, core = places()
    zero = slow >> 8
    fine = cos_sin((iota((8, 512), 1) * iota((8, 512), 0)) & (F - 1), F)
    blank = jnp.zeros((120, 128), f32)
    for part in range(2):
        for at in range(0, 512, 128):
            fine_ref[part, at : at + 128, :] = jnp.concatenate(
                [fine[part][:, at : at + 128], blank], axis=0
            ).T

    copies[0].wait()
    order = order_ref[...].astype(f32).astype(bf16)
    halves = []
    for c in range(2):
        owner = ((iota((128, 128), 1) & 31) << 3) + ((iota((128, 128), 1) >> 5) << 1) + c
        pick = iota((128, 128), 0) == (owner & 127)
        got = jnp.dot(order, pick.astype(f32).astype(bf16), preferred_element_type=f32)
        halves.append(jnp.where((iota((1, 128), 1) & 31) < 16, got[0:1], got[1:2]))
    flip = core == 0
    bands = jnp.concatenate(
        [jnp.where(flip, halves[1], halves[0]), jnp.where(flip, halves[0], halves[1])], axis=1
    ).astype(jnp.int32)

    steps = [(bands * k) & 3 for k in range(4)]
    real = [jnp.where(k == 0, 1.0, jnp.where(k == 2, -1.0, 0.0)) for k in steps]
    imag = [jnp.where(k == 1, 1.0, jnp.where(k == 3, -1.0, 0.0)) for k in steps]
    for at in range(0, 64, 16):
        c, s = cos_sin(((iota((16, BANDS), 0) + at) * bands) & (BANDS - 1), BANDS)
        band_ref[0, at : at + 16, :] = c
        band_ref[1, at : at + 16, :] = s
        for k in range(1, 4):
            band_ref[0, k * 64 + at : k * 64 + at + 16, :] = c * real[k] - s * imag[k]
            band_ref[1, k * 64 + at : k * 64 + at + 16, :] = s * real[k] + c * imag[k]

    def table(j, half, row):
        at = half * 256 + row
        fc = fine_ref[0, at : at + 16, j : j + 1]
        fs = fine_ref[1, at : at + 16, j : j + 1]
        bc = band_ref[0, row : row + 16, :]
        bs = band_ref[1, row : row + 16, :]
        c = (bc * fc - bs * fs).astype(bf16)
        s = (bs * fc + bc * fs).astype(bf16)
        if j % 2:
            wodd_ref[j // 2, at : at + 16, :] = c
            wodd_ref[j // 2, 512 + at : 512 + at + 16, :] = s
        else:
            weven_ref[j // 2, at : at + 16, :] = c
            weven_ref[j // 2, 256 + at : 256 + at + 16, :] = s

    def put(ref, index, row, col, depth, re, im):
        ref[index, row : row + 16, col : col + 128] = re
        ref[index, row : row + 16, depth + col : depth + col + 128] = im
        ref[index, 256 + row : 256 + row + 16, col : col + 128] = im
        ref[index, 256 + row : 256 + row + 16, depth + col : depth + col + 128] = -re

    def high(ref, index, row, col, depth, zr, zi):
        rh, ih = zr.astype(bf16), zi.astype(bf16)
        put(ref, index, row, col, depth, rh, ih)
        return zr - rh.astype(f32), zi - ih.astype(f32)

    def low(j, row, col, zr, zi):
        put(low_ref, j, row, col, 256, zr.astype(bf16), zi.astype(bf16))

    def quarters(g, part, cb):
        return [
            [
                x_ref[
                    g, c, part * 16 : part * 16 + 16, k * 512 + cb * 128 : k * 512 + cb * 128 + 128
                ].astype(f32)
                for k in range(4)
            ]
            for c in range(2)
        ]

    def fold_odd(g, part, pair):
        row = g * ROWS + part * 16
        rests = []
        for cb in (pair, pair + 2):
            re, im = quarters(g, part, cb)
            dr, di = re[0] - re[2], im[0] - im[2]
            er, ei = re[1] - re[3], im[1] - im[3]
            rests.append(
                (
                    high(odd_ref, 0, row, cb * 128, 512, dr + ei, di - er),
                    high(odd_ref, 1, row, cb * 128, 512, dr - ei, di + er),
                )
            )
        for q in range(2):
            (ar, ai), (br, bi) = rests[0][q], rests[1][q]
            cr, ci = (br + bi) * HALF_ROOT, (bi - br) * HALF_ROOT
            if q == 1:
                cr, ci = ci, -cr
            low(1 + 2 * q, row, pair * 128, ar + cr, ai + ci)
            low(5 + 2 * q, row, pair * 128, ar - cr, ai - ci)

    def fold_even(g, part, pair):
        row = g * ROWS + part * 16
        zs = []
        for cb in (pair, pair + 2):
            re, im = quarters(g, part, cb)
            sr, si = re[0] + re[2], im[0] + im[2]
            ur, ui = re[1] + re[3], im[1] + im[3]
            zs.append((sr + ur, si + ui, sr - ur, si - ui))
        (ar, ai, cr, ci), (br, bi, dr, di) = zs
        low(0, row, pair * 128, *high(even_ref, 0, row, pair * 128, 256, ar + br, ai + bi))
        low(4, row, pair * 128, *high(even_ref, 2, row, pair * 128, 256, ar - br, ai - bi))
        low(2, row, pair * 128, *high(even_ref, 1, row, pair * 128, 256, cr + di, ci - dr))
        low(6, row, pair * 128, *high(even_ref, 3, row, pair * 128, 256, cr - di, ci + dr))

    def walks_of():
        copies[1].wait()
        rows16 = iota((16, BANDS), 0) == (bands >> 4)
        pick = iota((128, BANDS), 0) == ((bands & 15) << 3)
        held = walk_ref[...].astype(f32)
        shifts = jnp.concatenate(
            [held if j == 0 else pltpu.roll(held, 128 - j, 1) for j in range(8)], axis=0
        )
        got = jnp.dot(
            shifts.astype(bf16), pick.astype(f32).astype(bf16), preferred_element_type=f32
        )
        walks = []
        for j in range(8):
            mine = jnp.where(rows16, got[j * 16 : j * 16 + 16], 0.0)
            walk = jnp.sum(mine, axis=0, keepdims=True).astype(jnp.int32)
            own_ref[j : j + 1, :] = walk[:, 128:]
            walks.append(walk)
        return walks

    def align(j, tile):
        lanes = slice(tile * 128, tile * 128 + 128)
        walk = walks[j][:, lanes]
        ahead = walk >= 0
        at = [(walk * (8 * slow + g)) >> 6 for g in range(PER)]
        rim = jnp.zeros((WIN - ROWS, 128), f32)
        total = None
        for i in range(PER):
            own = jnp.where(
                ahead,
                power_ref[j, i * ROWS : (i + 1) * ROWS, lanes],
                power_ref[j, (7 - i) * ROWS : (8 - i) * ROWS, lanes],
            )
            own = jnp.concatenate([own, rim], axis=0)
            if i == 0:
                total = own
            else:
                step = jnp.where(ahead, at[i] - at[i - 1], at[7 - i] - at[8 - i]) == 1
                total = jnp.where(step, pltpu.roll(total, 1, 0), total) + own
        if tile == 0:
            send_ref[j] = total
            return
        keep_ref[j] = total
        lower = slow & ~1
        apart = jnp.where(
            ahead,
            ((walk * (8 * lower + 15)) >> 6) - ((walk * (8 * lower + 7)) >> 6),
            ((walk * (8 * lower)) >> 6) - ((walk * (8 * lower + 8)) >> 6),
        )
        meet_ref[j : j + 1, :] = jnp.where(ahead, apart, -apart - 1)

    def products(pair, count, at, side):
        depth = 1024 if pair[0] % 2 else 512
        sums = [None, None]
        steps = [(0, k) for k in range(0, depth, 256)] + [(1, 0), (1, 256)]
        for done, (level, k) in enumerate(steps):
            for place, j in enumerate(pair):
                w_ref = wodd_ref if j % 2 else weven_ref
                table_row = k * (depth // 512) if level else k
                w = w_ref[j // 2, table_row : table_row + 256]
                if level:
                    left, index = low_ref, j
                elif j % 2:
                    left, index = odd_ref, (j // 2) % 2
                else:
                    left, index = even_ref, j // 2
                rows = jnp.concatenate(
                    [
                        left[index, at : at + count, k : k + 256],
                        left[index, 256 + at : 256 + at + count, k : k + 256],
                    ],
                    axis=0,
                )
                got = jnp.dot(rows, w, preferred_element_type=f32)
                sums[place] = got if sums[place] is None else sums[place] + got
            share = -(-len(side) // (len(steps) - done))
            for task in side[:share]:
                task()
            side = side[share:]
        for place, j in enumerate(pair):
            re, im = sums[place][:count], sums[place][count:]
            power_ref[j, at : at + count, :] = re * re + im * im

    def later(task, *args):
        return lambda: task(*args)

    def folds(task, batches, cuts):
        return [later(task, g, p, c) for g in batches for p in range(2) for c in range(cuts)]

    def aligns(*bins):
        return [later(align, j, tile) for j in bins for tile in range(2)]

    def tables(*bins):
        return [
            later(table, j, half, row)
            for j in bins
            for half in range(2 if j % 2 else 1)
            for row in range(0, 256, 16)
        ]

    for task in tables(1, 5):
        task()
    walks = walks_of()
    for g in range(4):
        copies[2 + g].wait()
    for task in folds(fold_odd, range(4), 2):
        task()
    for g in range(4, 8):
        copies[2 + g].wait()
    products((1, 5), 128, 0, folds(fold_odd, range(4, 8), 2) + tables(3, 7))
    products((1, 5), 128, 128, folds(fold_even, range(8), 2))
    products((3, 7), 256, 0, tables(0, 4, 2, 6) + aligns(1, 5))
    products((0, 4), 256, 0, aligns(3, 7))
    products((2, 6), 256, 0, aligns(0, 4))
    for task in aligns(2, 6):
        task()


def pair_kernel(mine_ref, theirs_ref, meet_ref, out_ref, flat_ref):
    first = lax.axis_index("c") == 0
    for j in range(8):
        mine = mine_ref[j]
        theirs = theirs_ref[j]
        lower = jnp.where(first, mine, theirs)
        upper = jnp.where(first, theirs, mine)
        meet = meet_ref[j : j + 1, :]
        ahead = meet >= 0
        apart = jnp.where(ahead, meet, -meet - 1)
        moved = jnp.where(ahead, lower, upper)
        still = jnp.where(ahead, upper, lower)
        for bit in range(3):
            moved = jnp.where(((apart >> bit) & 1) == 1, pltpu.roll(moved, 1 << bit, 0), moved)
        flat_ref[j * WIN : (j + 1) * WIN, :] = moved + still
    flat_ref[8 * WIN :, :] = jnp.zeros((64, 128), f32)
    for piece in range(3):
        part = slice(piece * 128, (piece + 1) * 128)
        out_ref[:, part] = flat_ref[part, :].T


def join_kernel(walk_ref, x_ref, out_ref, turned_ref):
    lane = iota((1, 128), 1)
    group = lane // 32
    block = lane & 31
    here = lax.axis_index("x") * 32 + lax.axis_index("z") * 4 + lax.axis_index("y")
    walk = jnp.sum(jnp.where(lane == here, walk_ref[...], 0), axis=1, keepdims=True)
    batch = 16 * group + jnp.where(walk >= 0, 15, 0)
    moves = 32 - ((walk * batch) >> 6)
    flat = jnp.concatenate(
        [x_ref[:, piece * 128 : (piece + 1) * 128].T for piece in range(3)], axis=0
    )
    for quad in range(2):
        packed = None
        for jq in range(4):
            j = quad * 4 + jq
            move = moves[j : j + 1, :]
            current = jnp.concatenate(
                [flat[j * WIN : (j + 1) * WIN], jnp.zeros((8, 128), f32)], axis=0
            )
            for bit in range(6):
                taken = ((move >> bit) & 1) == 1
                if bit < 3:
                    current = jnp.where(taken, pltpu.roll(current, 1 << bit, 0), current)
                else:
                    pad = jnp.zeros((1 << bit, 128), f32)
                    low = jnp.concatenate([current, pad], axis=0)
                    high = jnp.concatenate([pad, current], axis=0)
                    current = jnp.where(taken, high[:96], low[:96])
            current = current + pltpu.roll(current, 64, 1)
            current = current + pltpu.roll(current, 32, 1)
            before = jnp.where(block == 31, 0.0, pltpu.roll(current[0:32], 127, 1))
            after = jnp.where(block == 0, 0.0, pltpu.roll(current[64:96], 1, 1))
            summed = before + current[32:64] + after
            packed = summed if packed is None else jnp.where(group == jq, summed, packed)
        packed = packed * SCALE
        turned_ref[quad * 128 : (quad + 1) * 128, :] = jnp.concatenate([packed] * 4, axis=0).T
    for v in range(8):
        result = None
        for c in range(4):
            piece = turned_ref[pl.ds(4 * v + c, 8, stride=32), :]
            result = piece if result is None else jnp.where(group == c, piece, result)
        out_ref[:, v * 128 : (v + 1) * 128] = result


VM = pl.BlockSpec(memory_space=pltpu.VMEM)


def on_device(profiles, range_walk, band_order):
    block = jax.ShapeDtypeStruct((8, WIN, 128), f32)
    row = jax.ShapeDtypeStruct((8, 128), jnp.int32)
    ANY = pl.BlockSpec(memory_space=pltpu.HBM)
    send, keep, meet, walks = pl.pallas_call(
        spectra_kernel,
        out_shape=(block, block, row, row),
        in_specs=[ANY, ANY, ANY],
        out_specs=(VM, VM, VM, VM),
        scratch_shapes=[
            pltpu.VMEM((PER, 2, ROWS, F), bf16),
            pltpu.VMEM((2, 128), jnp.int32),
            pltpu.VMEM((16, 128), jnp.int32),
            pltpu.VMEM((2, BANDS, BANDS), f32),
            pltpu.VMEM((2, 512, 128), f32),
            pltpu.VMEM((8, 256, 256), f32),
            pltpu.SemaphoreType.DMA((2 + PER,)),
        ],
        compiler_params=pltpu.CompilerParams(vmem_limit_bytes=GRANT),
    )(
        *(
            pltpu.with_memory_space_constraint(array, pltpu.HBM)
            for array in (profiles, band_order.reshape(2, 128), range_walk.reshape(16, 128))
        )
    )
    theirs = lax.ppermute(send, "c", [(0, 1), (1, 0)])
    messages = pl.pallas_call(
        pair_kernel,
        out_shape=jax.ShapeDtypeStruct((128, 384), f32),
        in_specs=[VM, VM, VM],
        out_specs=VM,
        scratch_shapes=[pltpu.VMEM((384, 128), f32)],
        compiler_params=pltpu.CompilerParams(vmem_limit_bytes=4 << 20),
    )(keep, theirs, meet)
    arrived = lax.all_to_all(
        messages.reshape(128, 1, 384), ("x", "z", "y"), split_axis=0, concat_axis=0, tiled=True
    )
    return pl.pallas_call(
        join_kernel,
        out_shape=jax.ShapeDtypeStruct((8, 1024), f32),
        in_specs=[VM, VM],
        out_specs=VM,
        scratch_shapes=[pltpu.VMEM((256, 128), f32)],
        compiler_params=pltpu.CompilerParams(vmem_limit_bytes=4 << 20),
    )(walks, arrived.reshape(128, 384))


def solution(mesh):
    fine = Mesh(mesh.devices.reshape(8, 4, 4, 2), ("z", "y", "x", "c"))
    placed = (P(("x", "c"), None, ("z", "y"), None), P(), P())
    return jax.shard_map(
        on_device, mesh=fine, in_specs=placed, out_specs=P(("z", "y", "x", "c"), None), check_vma=False
    )
```
